128 devices in a mesh: seq: 32 (over y, z, core), batch: 4 (over x).
Axes of the slice: x: 4, y: 4, z: 4, core: 2. Of those that a mesh axis runs over, the one named last changes fastest.
Arguments:
- queries: bfloat16 [4, 4096, 4096], P('batch', 'seq'), may hold values from -130 to 130
- keys: bfloat16 [4, 4096, 1024], P('batch', 'seq'), may hold values from -4 to 4
- values: bfloat16 [4, 4096, 1024], P('batch', 'seq'), may hold values from -4 to 4
- lengths: int32 [4], P('batch'), may hold values from 2048 to 4096
- block_pos: int32 [4, 32], P('batch'), may hold values from 0 to 31, each once within a row
- w_in: bfloat16 [6144, 1024], replicated, may hold values from -0.078125 to 0.078125
- b_in: float32 [1024], replicated, may hold values from -3 to 3
- output_weight: bfloat16 [1024, 8], replicated, may hold values from -0.1875 to 0.1875
- output_bias: float32 [8], replicated, may hold values from 1 to 2
Outputs:
- grad_w_in: float32 [6144, 1024], P(('seq', 'batch'))
- grad_b_in: float32 [1024], replicated
- output_weight_gradient: float32 [1024, 8], replicated
- output_bias_gradient: float32 [8], replicated
The draws below stay inside these ranges and needn't reach their ends.
Inputs may be any that keep to these rules, and one draw needn't show every extreme that they name: Each row of block_pos names every block 0 to 31 once.
All inputs are finite; a program needn't handle non-finite values.
Results may differ from the reference program's by a relative error of at most 0.0017.
The reference program's roundings to bfloat16 on the way (of `features`, `act`, `resid` and `delta`) count: a program that leaves them out, or rounds other values in their place, can miss the bound.
Values may be sent and summed in bfloat16 or wider, within the bound.
A program may use at most 128 MiB of HBM per device.

```python
import math
import jax
import jax.numpy as jnp
from jax import lax

QUERY_HEADS = 32
KEY_VALUE_HEADS = 8
HEAD_DIMENSION = 128
HIDDEN_UNITS = 1024
SEQ_DEV = 128
KD = 1024
FEAT = 6144
TOKEN_COUNT = 4096
SEQUENCE_COUNT = 4
N_SEQ = 32


def group_keys(key):
    base_offset = jax.random.fold_in(key, 7301)
    return jnp.clip(jax.random.normal(base_offset, (SEQUENCE_COUNT, TOKEN_COUNT, KEY_VALUE_HEADS * HEAD_DIMENSION), jnp.float32), -4.0, 4.0)


def draw_keys(key, part):
    base_offset = group_keys(key)
    return base_offset.astype(jnp.bfloat16)


def draw_queries(key, part):
    fresh = jax.random.fold_in(key, 1709)
    base_offset = jnp.clip(jax.random.normal(fresh, (SEQUENCE_COUNT, TOKEN_COUNT, QUERY_HEADS * HEAD_DIMENSION), jnp.float32), -4.0, 4.0)
    return base_offset.astype(jnp.bfloat16)


def place_ends(entries, stream_key, least, largest):
    index_at = [jax.random.randint(jax.random.fold_in(stream_key, axis), (), 0, length) for axis, length in enumerate(entries.shape)]
    widest = entries.shape.index(max(entries.shape))
    next_to = index_at[:widest] + [(index_at[widest] + 1) % entries.shape[widest]] + index_at[widest + 1:]
    return entries.at[tuple(index_at)].set(least).at[tuple(next_to)].set(largest)


def shard_levels(stream_key, shape, pieces, least, high):
    gain = 1.0
    for dim, blocks in pieces:
        steps = jax.random.uniform(jax.random.fold_in(jax.random.fold_in(stream_key, 6), dim), (blocks,), jnp.float32, least / len(pieces), high / len(pieces))
        gain = gain * jnp.repeat(jnp.exp(steps), shape[dim] // blocks).reshape((-1,) + (1,) * (len(shape) - 1 - dim))
    return gain


def bell_draw(stream_key, dims, scale, most, split=(), kind=jnp.bfloat16):
    array = jax.random.normal(stream_key, dims, jnp.float32) * scale
    if len(split) > 0:
        array = shard_levels(stream_key, dims, split, -0.22, 0.18) * array
    return jnp.clip(array, min=-most, max=most).astype(kind)


def setup_inputs(seed: int = 0) -> dict:
    seeds = jax.random.split(jax.random.key(seed), 10)
    queries = draw_queries(jax.random.fold_in(seeds[9], 71), 0)
    keys = draw_keys(jax.random.fold_in(seeds[9], 71), 0)
    values = bell_draw(seeds[2], (SEQUENCE_COUNT, TOKEN_COUNT, KD), 1.0, 4.0, ((0, 4), (1, 32)))
    lengths = place_ends(jax.random.randint(seeds[3], (SEQUENCE_COUNT,), TOKEN_COUNT // 2, TOKEN_COUNT + 1), jax.random.fold_in(seeds[3], 1), TOKEN_COUNT // 2, TOKEN_COUNT).astype(jnp.int32)
    block_pos = jax.vmap(lambda own: jax.random.permutation(own, N_SEQ))(jax.random.split(seeds[4], SEQUENCE_COUNT)).reshape((SEQUENCE_COUNT, N_SEQ)).astype(jnp.int32)
    w_in = bell_draw(seeds[5], (FEAT, HIDDEN_UNITS), FEAT ** -0.5, 0.078125)
    b_in = bell_draw(seeds[6], (HIDDEN_UNITS,), 0.5, 3.0, (), jnp.float32)
    output_weight = bell_draw(seeds[7], (HIDDEN_UNITS, KEY_VALUE_HEADS), HIDDEN_UNITS ** -0.5, 0.1875)
    output_bias = jnp.clip(jax.random.uniform(seeds[8], (KEY_VALUE_HEADS,), jnp.float32, 1.0, 2.0), 1.0, 2.0)
    return {"queries": queries, "keys": keys, "values": values, "lengths": lengths, "block_pos": block_pos, "w_in": w_in, "b_in": b_in, "output_weight": output_weight, "output_bias": output_bias}


def column_mass(q_rows, k_rows, positions, limit):
    group_index = QUERY_HEADS // KEY_VALUE_HEADS
    scale = 1.0 / math.sqrt(HEAD_DIMENSION)

    def queries_per_group(g, sums):
        g32 = jnp.asarray(g).astype(jnp.int32)
        k_part = lax.dynamic_slice_in_dim(k_rows, g32 * HEAD_DIMENSION, HEAD_DIMENSION, 1).astype(jnp.float32)
        key_live = positions < limit

        def per_block(i, column):
            i32 = jnp.asarray(i).astype(jnp.int32)
            start = i32 * SEQ_DEV
            q_part = lax.dynamic_slice(q_rows, (start, g32 * group_index * HEAD_DIMENSION), (SEQ_DEV, group_index * HEAD_DIMENSION))
            q_part = q_part.astype(jnp.float32).reshape(SEQ_DEV, group_index, HEAD_DIMENSION)
            q_pos = lax.dynamic_slice_in_dim(positions, start, SEQ_DEV)
            allowed = (positions[None, :] <= q_pos[:, None]) & key_live[None, :]
            scores = jnp.einsum('qhd,kd->hqk', q_part, k_part) * scale
            masked = jnp.where(allowed[None], scores, -1e+30)
            top = lax.optimization_barrier(jnp.max(masked, axis=2, keepdims=True))
            weights = jnp.where(allowed[None], jnp.exp(masked - top), 0.0)
            total = lax.optimization_barrier(jnp.sum(weights, axis=2, keepdims=True))
            q_live = (q_pos < limit).astype(jnp.float32)
            share = weights / total * q_live[None, :, None]
            return column + lax.optimization_barrier(jnp.sum(share, axis=(0, 1)))
        column = lax.fori_loop(0, N_SEQ, per_block, jnp.zeros((TOKEN_COUNT,), jnp.float32))
        return lax.dynamic_update_index_in_dim(sums, column, g32, 0)
    return lax.fori_loop(0, KEY_VALUE_HEADS, queries_per_group, jnp.zeros((KEY_VALUE_HEADS, TOKEN_COUNT), jnp.float32))

def reference(queries, keys, values, lengths, block_pos, w_in, b_in, output_weight, output_bias):
    norm = 1.0 / math.sqrt(SEQUENCE_COUNT * TOKEN_COUNT)
    offsets = jnp.arange(SEQ_DEV, dtype=jnp.int32)
    grad_w_in = jnp.zeros((FEAT, HIDDEN_UNITS), jnp.float32)
    grad_b_in = jnp.zeros((HIDDEN_UNITS,), jnp.float32)
    output_weight_gradient = jnp.zeros((HIDDEN_UNITS, KEY_VALUE_HEADS), jnp.float32)
    output_bias_gradient = jnp.zeros((KEY_VALUE_HEADS,), jnp.float32)
    for index in range(SEQUENCE_COUNT):
        q_rows = queries[index]
        k_rows = keys[index]
        v_rows = values[index]
        positions = (block_pos[index][:, None] * SEQ_DEV + offsets[None, :]).reshape(-1).astype(jnp.int32)
        limit = lengths[index]
        live = (positions < limit).astype(jnp.float32)
        mass = column_mass(q_rows, k_rows, positions, limit)
        labels = jnp.log1p(mass).T
        features = jnp.concatenate([q_rows, k_rows, v_rows], axis=1)
        pre = jnp.dot(features, w_in, preferred_element_type=jnp.float32) + b_in
        act = jax.nn.silu(pre).astype(jnp.bfloat16)
        pred = jnp.dot(act, output_weight, preferred_element_type=jnp.float32) + output_bias
        resid = ((pred - labels) * live[:, None] * norm).astype(jnp.bfloat16)
        back = jnp.dot(resid, output_weight.T, preferred_element_type=jnp.float32)
        sig = jax.nn.sigmoid(pre)
        delta = (back * sig * (1.0 + pre * (1.0 - sig))).astype(jnp.bfloat16)
        grad_w_in = grad_w_in + jnp.dot(features.T, delta, preferred_element_type=jnp.float32)
        grad_b_in = grad_b_in + lax.optimization_barrier(jnp.sum(delta.astype(jnp.float32), axis=0))
        output_weight_gradient = output_weight_gradient + jnp.dot(act.T, resid, preferred_element_type=jnp.float32)
        output_bias_gradient = output_bias_gradient + lax.optimization_barrier(jnp.sum(resid.astype(jnp.float32), axis=0))
    return (grad_w_in, grad_b_in, output_weight_gradient, output_bias_gradient)
```

```python
import functools
import math

import jax
import jax.numpy as jnp
from jax import lax
from jax.experimental import pallas as pl
from jax.experimental.pallas import tpu as pltpu
from jax.sharding import PartitionSpec as P

MESH = pl.DeviceIdType.MESH
F32 = jnp.float32
BF16 = jnp.bfloat16
VM = pltpu.VMEM
CK = 512
WK = 512


def place():
    seq = lax.axis_index("seq")
    x = lax.axis_index("batch")
    y = seq // 8
    row = lax.rem(seq, 8)
    core = lax.rem(seq, 2)
    return seq, x, y, row, core


def greet(seq, x, y, row, core):
    bar = pltpu.get_barrier_semaphore()
    n = 0
    for k in range(1, 8):
        pl.semaphore_signal(
            bar, inc=1, device_id=(y * 8 + lax.rem(row + k, 8), x), device_id_type=MESH
        )
        n += 1
    for k in range(1, 4):
        pl.semaphore_signal(
            bar, inc=1, device_id=(lax.rem(y + k, 4) * 8 + row, x), device_id_type=MESH
        )
        n += 1
    for k in range(1, 8):
        pl.semaphore_signal(bar, inc=1, device_id=group_peer(seq, x, core, k), device_id_type=MESH)
        n += 1
    pl.semaphore_wait(bar, n)


def group_rank(x, core):
    return core * 4 + x


def group_peer(seq, x, core, k):
    j = lax.rem(group_rank(x, core) + k, 8)
    return (seq - core + j // 4, lax.rem(j, 4))


def remote(src, dst, ss, rs, dev):
    return pltpu.make_async_remote_copy(
        src_ref=src, dst_ref=dst, send_sem=ss, recv_sem=rs, device_id=dev, device_id_type=MESH
    )


def spread_kernel(
    q, k, v, w_hbm, b_in, wo, bo, qg, kg, ft_all, sp, act, pred,
    ft, wbuf, pre, wsem, ks, kr, qs, qr, fs, fr, ys, yr, ls,
):
    seq, x, y, row, core = place()
    j = group_rank(x, core)
    chunks = w_hbm.shape[0] // WK

    def fetch(i):
        return pltpu.make_async_copy(
            w_hbm.at[pl.ds(i * WK, WK)], wbuf.at[i % 3], wsem.at[i % 3]
        )

    fetch(0).start()
    fetch(1).start()
    greet(seq, x, y, row, core)
    kc, qc, fc, yc = [], [], [], []
    for n in range(1, 8):
        to = lax.rem(row + n, 8)
        c = remote(
            k.at[:, pl.ds(pl.multiple_of(to * 128, 128), 128)], kg.at[seq],
            ks.at[n], kr.at[n], (y * 8 + to, x),
        )
        c.start()
        kc.append(c)
    for n in range(1, 8):
        to = lax.rem(row + n, 8)
        c = remote(
            q.at[:, pl.ds(pl.multiple_of(to * 512, 512), 512)], qg.at[row],
            qs.at[n], qr.at[n], (y * 8 + to, x),
        )
        c.start()
        qc.append(c)
    own_k = pltpu.make_async_copy(
        k.at[:, pl.ds(pl.multiple_of(row * 128, 128), 128)], kg.at[seq], ls.at[0]
    )
    own_q = pltpu.make_async_copy(
        q.at[:, pl.ds(pl.multiple_of(row * 512, 512), 512)], qg.at[row], ls.at[1]
    )
    own_k.start()
    own_q.start()
    for i in range(16):
        src, lo = (q, i * 384)
        parts = []
        for t in range(3):
            col = lo + t * 128
            if col < 4096:
                parts.append(q[:, col : col + 128])
            elif col < 5120:
                parts.append(k[:, col - 4096 : col - 3968])
            else:
                parts.append(v[:, col - 5120 : col - 4992])
        block = jnp.concatenate(parts, axis=1).astype(F32).T.astype(BF16)
        for t in range(8):
            ft[i, t] = block[t * 48 : (t + 1) * 48]
    lanes = pl.ds(pl.multiple_of(j * 128, 128), 128)
    for n in range(1, 8):
        to = lax.rem(j + n, 8)
        c = remote(
            ft.at[:, to], ft_all.at[:, :, lanes], fs.at[n], fr.at[n], group_peer(seq, x, core, n)
        )
        c.start()
        fc.append(c)
    own_f = pltpu.make_async_copy(ft.at[:, j], ft_all.at[:, :, lanes], ls.at[2])
    own_f.start()

    def multiply(i):
        if i + 2 < chunks:
            fetch(i + 2).start()
        fetch(i).wait()
        lo = i * WK
        if lo < 4096:
            a = q[:, lo : lo + WK]
        elif lo < 5120:
            a = k[:, lo - 4096 : lo - 4096 + WK]
        else:
            a = v[:, lo - 5120 : lo - 5120 + WK]
        part = jnp.dot(a, wbuf[i % 3], preferred_element_type=F32)
        pre[...] = part if i == 0 else pre[...] + part

    for i in range(chunks // 2):
        multiply(i)
    for c in kc:
        c.wait()
    own_k.wait()
    mine = kg.at[pl.ds(y * 8, 8)]
    for n in range(1, 4):
        c = remote(mine, mine, ys.at[n], yr.at[n], (lax.rem(y + n, 4) * 8 + row, x))
        c.start()
        yc.append(c)
    for i in range(chunks // 2, chunks):
        multiply(i)
    z = pre[...] + b_in[...]
    sig = jax.nn.sigmoid(z)
    a = (z * sig).astype(BF16)
    act[...] = a
    sp[...] = sig * (1.0 + z * (1.0 - sig))
    pred[...] = lax.dot_general(
        wo[...], a, (((1,), (1,)), ((), ())), preferred_element_type=F32
    )[0:8] + bo[...]
    for c in qc + fc + yc:
        c.wait()
    own_q.wait()
    own_f.wait()


def spread(q, k, v, w, b_in, wo, bo):
    dma = pltpu.SemaphoreType.DMA
    vmem = pl.BlockSpec(memory_space=VM)
    return pl.pallas_call(
        spread_kernel,
        name="spread",
        out_shape=(
            jax.ShapeDtypeStruct((8, 128, 512), BF16),
            jax.ShapeDtypeStruct((32, 128, 128), BF16),
            jax.ShapeDtypeStruct((16, 48, 1024), BF16),
            jax.ShapeDtypeStruct((128, 1024), F32),
            jax.ShapeDtypeStruct((128, 1024), BF16),
            jax.ShapeDtypeStruct((8, 128), F32),
        ),
        in_specs=[vmem, vmem, vmem, pl.BlockSpec(memory_space=pl.ANY), vmem, vmem, vmem],
        out_specs=(vmem,) * 6,
        scratch_shapes=[
            VM((16, 8, 48, 128), BF16),
            VM((3, WK, 1024), BF16),
            VM((128, 1024), F32),
            dma((3,)),
            dma((8,)), dma((8,)), dma((8,)), dma((8,)), dma((8,)), dma((8,)), dma((4,)), dma((4,)),
            dma((3,)),
        ],
        compiler_params=pltpu.CompilerParams(
            collective_id=0, has_side_effects=True, vmem_limit_bytes=48 * 2**20
        ),
    )(q, k, v, w, b_in, wo, bo)


def mass_kernel(meta, qg, kg, out, kpos, s_ref, acc):
    limit = meta[32]
    first = meta[33]
    factor = math.log2(math.e) / math.sqrt(128)

    def order(r, _):
        kpos[pl.ds(pl.multiple_of(meta[r] * 128, 128), 128)] = kg[r]
        return 0

    lax.fori_loop(0, 32, order, 0)
    acc[...] = jnp.zeros_like(acc)
    lane = lax.rem(lax.broadcasted_iota(jnp.int32, (1, 512), 1), 128)
    sub = lax.broadcasted_iota(jnp.int32, (CK, 512), 0)

    def fold(a, op):
        return op(a.reshape(CK // 8, 8, 512), axis=0)

    def block(i, _):
        pos = meta[first + i]

        @pl.when(pos * 128 < limit)
        def _():
            last = pos * 128 // CK
            q4 = jnp.concatenate([qg[i, :, h * 128 : (h + 1) * 128] for h in range(4)], axis=0)

            def scores(c):
                rows = pl.ds(pl.multiple_of(c * CK, CK), CK)
                return rows, lax.dot_general(
                    kpos[rows], q4, (((1,), (1,)), ((), ())), preferred_element_type=F32
                )

            def first_pass(c, top):
                rows, s = scores(c)
                s_ref[rows] = s
                return jnp.maximum(top, fold(s, jnp.max))

            top = lax.fori_loop(0, last, first_pass, jnp.full((8, 512), -1e30, F32))
            rows, s = scores(last)
            s = jnp.where(sub + last * CK <= lane + pos * 128, s, -1e30)
            s_ref[rows] = s
            top = jnp.max(jnp.maximum(top, fold(s, jnp.max)), axis=0, keepdims=True)

            def second_pass(c, total):
                rows = pl.ds(pl.multiple_of(c * CK, CK), CK)
                e = jnp.exp2((s_ref[rows] - top) * factor)
                s_ref[rows] = e
                return total + fold(e, jnp.sum)

            total = lax.fori_loop(0, last + 1, second_pass, jnp.zeros((8, 512), F32))
            total = jnp.sum(total, axis=0, keepdims=True)
            share = jnp.where(lane + pos * 128 < limit, 1.0 / total, 0.0)

            def third_pass(c, _):
                rows = pl.ds(pl.multiple_of(c * CK, CK), CK)
                e = s_ref[rows] * share
                acc[rows] += (e[:, 0:128] + e[:, 128:256]) + (e[:, 256:384] + e[:, 384:512])
                return 0

            lax.fori_loop(0, last + 1, third_pass, 0)

        return 0

    lax.fori_loop(0, 8, block, 0)

    def give(r, _):
        rows = acc[pl.ds(pl.multiple_of(meta[r] * 128, 128), 128)]
        out[pl.ds(r, 1)] = jnp.sum(rows.T, axis=0, keepdims=True)
        return 0

    lax.fori_loop(0, 32, give, 0)


def column_mass(meta, qg, kg):
    vmem = pl.BlockSpec(memory_space=VM)
    return pl.pallas_call(
        mass_kernel,
        name="column_mass",
        out_shape=jax.ShapeDtypeStruct((32, 128), F32),
        in_specs=[pl.BlockSpec(memory_space=pltpu.SMEM), vmem, vmem],
        out_specs=vmem,
        scratch_shapes=[VM((4096, 128), BF16), VM((4096, 512), F32), VM((4096, 128), F32)],
        compiler_params=pltpu.CompilerParams(vmem_limit_bytes=48 * 2**20),
    )(meta, qg, kg)


def reduce_kernel(
    norm, mass, sp, act, pred, live, wo, ft, out, small,
    m1, m2s, m2, dl, ga, gb, own_a, own_b, ra, rb, pa, pb, ta, tb,
    pk, p1, p2, p3,
    s1, r1, s2, r2, s3, r3, s4, r4, s5, r5, sa, qa, sb, qb, s6, r6, s7, r7, s8, r8, s9, r9,
):
    seq, x, y, row, core = place()
    z = row // 2
    j = group_rank(x, core)
    greet(seq, x, y, row, core)

    def y_dev(n):
        return (lax.rem(y + n, 4) * 8 + row, x)

    def z_dev(n):
        return (y * 8 + lax.rem(z + n, 4) * 2 + core, x)

    cs = []
    for n in range(1, 4):
        c = remote(mass.at[lax.rem(y + n, 4)], m1.at[y], s1.at[n], r1.at[n], y_dev(n))
        c.start()
        cs.append(c)
    m1[y] = mass[y]
    for c in cs:
        c.wait()
    total = (m1[0] + m1[1]) + (m1[2] + m1[3])
    for i in range(8):
        m2s[i] = jnp.broadcast_to(total[i : i + 1], (8, 128))
    cs = []
    for n in range(1, 8):
        to = lax.rem(row + n, 8)
        c = remote(m2s.at[to], m2.at[row], s2.at[n], r2.at[n], (y * 8 + to, x))
        c.start()
        cs.append(c)
    m2[row] = m2s[row]
    for c in cs:
        c.wait()
    label = jnp.concatenate([jnp.log1p(m2[i, 0:1]) for i in range(8)], axis=0)
    resid = ((pred[...] - label) * live[...] * norm).astype(BF16).astype(F32)
    wide = jnp.concatenate([resid, jnp.zeros((120, 128), F32)], axis=0)
    back = jnp.dot(wide.T.astype(BF16), wo[...], preferred_element_type=F32)
    delta = (back * sp[...]).astype(BF16)
    dl[j] = delta
    step = 1 - 2 * core
    ahead = lax.rem(x + step + 4, 4)
    behind = lax.rem(x - step + 4, 4)
    far = lax.rem(x + 2, 4)
    other = (seq + step, x)

    def give(slot, n, dev):
        return remote(dl.at[slot], dl.at[slot], s3.at[n], r3.at[n], dev)

    base = core * 4
    g_a = give(j, 0, (seq, ahead))
    g_b = give(j, 1, (seq, behind))
    h_0 = give(j, 3, other)
    g_a.start()
    g_b.start()
    h_0.start()
    termT = jnp.dot(wide.astype(BF16), act[...], preferred_element_type=F32)[0:8]
    bias = jnp.sum(delta.astype(F32), axis=0, keepdims=True)
    for i in range(4):
        pk[i] = termT[:, i * 256 : (i + 1) * 256]
    pk[4, :, 0:128] = resid
    for i in range(8):
        pk[4, i : i + 1, 128:256] = bias[:, i * 128 : (i + 1) * 128]
    for i in range(5, 8):
        pk[i] = jnp.zeros((8, 256), F32)
    cs = []
    for n in range(1, 8):
        c = remote(
            pk.at[lax.rem(j + n, 8)], p1.at[j], s4.at[n], r4.at[n], group_peer(seq, x, core, n)
        )
        c.start()
        cs.append(c)
    p1[j] = pk[j]
    g_a.wait_recv()
    g_c = give(base + behind, 2, (seq, ahead))
    g_c.start()
    h_1 = give(base + behind, 4, other)
    h_1.start()
    g_b.wait_recv()
    h_2 = give(base + ahead, 5, other)
    h_2.start()
    for c in cs:
        c.wait()
    t = p1[0]
    for i in range(1, 8):
        t = t + p1[i]
    p2[y] = t
    cs = []
    for n in range(1, 4):
        c = remote(p2.at[y], p2.at[y], s5.at[n], r5.at[n], y_dev(n))
        c.start()
        cs.append(c)
    g_c.wait_recv()
    h_3 = give(base + far, 6, other)
    h_3.start()
    for c in cs:
        c.wait()
    p3[z] = (p2[0] + p2[1]) + (p2[2] + p2[3])
    zs = []
    for n in range(1, 4):
        c = remote(p3.at[z], p3.at[z], s6.at[n], r6.at[n], z_dev(n))
        c.start()
        zs.append(c)
    for c in (h_0, h_1, h_2, h_3):
        c.wait()
    g_a.wait_send()
    g_b.wait_send()
    g_c.wait_send()

    d_all = dl[...].reshape(1024, 1024)
    f_all = ft[...].reshape(768, 1024)
    a_all = jnp.dot(f_all, d_all[:, 0:512], preferred_element_type=F32).reshape(4, 4, 48, 512)
    ga[...] = a_all.astype(BF16)
    own_a[...] = a_all
    acs = []
    for n in range(1, 4):
        c = remote(ga.at[lax.rem(y + n, 4)], ra.at[y], sa.at[n], qa.at[n], y_dev(n))
        c.start()
        acs.append(c)
    b_all = jnp.dot(f_all, d_all[:, 512:1024], preferred_element_type=F32).reshape(4, 4, 48, 512)
    gb[...] = b_all.astype(BF16)
    own_b[...] = b_all
    bcs = []
    for n in range(1, 4):
        c = remote(gb.at[:, lax.rem(z + n, 4)], rb.at[z], sb.at[n], qb.at[n], z_dev(n))
        c.start()
        bcs.append(c)
    for c in zs:
        c.wait()
    small[j] = (p3[0] + p3[1]) + (p3[2] + p3[3])
    fin = []
    for n in range(1, 8):
        c = remote(
            small.at[j], small.at[j], s7.at[n], r7.at[n], group_peer(seq, x, core, n)
        )
        c.start()
        fin.append(c)
    for c in acs:
        c.wait()
    sum_a = own_a[y]
    for n in range(1, 4):
        sum_a = sum_a + ra[lax.rem(y + n, 4)].astype(F32)
    pa[...] = sum_a
    acs = []
    for n in range(1, 4):
        c = remote(pa.at[lax.rem(z + n, 4)], ta.at[z], s8.at[n], r8.at[n], z_dev(n))
        c.start()
        acs.append(c)
    for c in bcs:
        c.wait()
    sum_b = own_b[:, z]
    for n in range(1, 4):
        sum_b = sum_b + rb[lax.rem(z + n, 4)].astype(F32)
    pb[...] = sum_b
    bcs = []
    for n in range(1, 4):
        c = remote(pb.at[lax.rem(y + n, 4)], tb.at[y], s9.at[n], r9.at[n], y_dev(n))
        c.start()
        bcs.append(c)
    for c in acs:
        c.wait()
    t = pa[z]
    for n in range(1, 4):
        t = t + ta[lax.rem(z + n, 4)]
    out[:, 0:512] = t
    for c in bcs:
        c.wait()
    t = pb[y]
    for n in range(1, 4):
        t = t + tb[lax.rem(y + n, 4)]
    out[:, 512:1024] = t
    for c in fin:
        c.wait()


def reduce_all(norm, mass, sp, act, pred, live, wo, ft):
    dma = pltpu.SemaphoreType.DMA
    vmem = pl.BlockSpec(memory_space=VM)
    return pl.pallas_call(
        functools.partial(reduce_kernel, norm),
        name="reduce_all",
        out_shape=(
            jax.ShapeDtypeStruct((48, 1024), F32),
            jax.ShapeDtypeStruct((8, 8, 256), F32),
        ),
        in_specs=[vmem] * 7,
        out_specs=(vmem,) * 2,
        scratch_shapes=[
            VM((4, 8, 128), F32), VM((8, 8, 128), F32), VM((8, 8, 128), F32),
            VM((8, 128, 1024), BF16),
            VM((4, 4, 48, 512), BF16), VM((4, 4, 48, 512), BF16),
            VM((4, 4, 48, 512), F32), VM((4, 4, 48, 512), F32),
            VM((4, 4, 48, 512), BF16), VM((4, 4, 48, 512), BF16),
            VM((4, 48, 512), F32), VM((4, 48, 512), F32),
            VM((4, 48, 512), F32), VM((4, 48, 512), F32),
            VM((8, 8, 256), F32), VM((8, 8, 256), F32), VM((4, 8, 256), F32), VM((4, 8, 256), F32),
        ]
        + [dma((4,)), dma((4,)), dma((8,)), dma((8,)), dma((8,)), dma((8,)), dma((8,)), dma((8,))]
        + [dma((4,)), dma((4,)), dma((4,)), dma((4,)), dma((4,)), dma((4,)), dma((4,)), dma((4,))]
        + [dma((8,)), dma((8,)), dma((4,)), dma((4,)), dma((4,)), dma((4,))],
        compiler_params=pltpu.CompilerParams(
            collective_id=1, has_side_effects=True, vmem_limit_bytes=56 * 2**20
        ),
    )(mass, sp, act, pred, live, wo, ft)


def on_device(queries, keys, values, lengths, block_pos, w_in, b_in, output_weight, output_bias):
    seq = lax.axis_index("seq")
    order = block_pos[0]
    limit = lengths[0]
    wo = jnp.pad(output_weight.T, ((0, 120), (0, 0)))
    bo = jnp.broadcast_to(output_bias[:, None], (8, 128))
    meta = jnp.concatenate(
        [order, limit[None], (seq // 8 * 8)[None].astype(jnp.int32), jnp.zeros((94,), jnp.int32)]
    )
    offsets = jnp.arange(128, dtype=jnp.int32)
    mine = lax.dynamic_index_in_dim(order, seq, 0, keepdims=False) * 128 + offsets
    live = (mine < limit).astype(F32)[None, :]
    norm = 1.0 / math.sqrt(4 * 4096)
    qg, kg, ft, sp, act, pred = spread(
        queries[0], keys[0], values[0], w_in, b_in[None, :], wo, bo
    )
    mass = column_mass(meta, qg, kg)
    grad, small = reduce_all(norm, mass.reshape(4, 8, 128), sp, act, pred, live, wo, ft)
    term = jnp.concatenate([small[i] for i in range(4)], axis=1).T
    bias = small[4, :, 128:256].reshape(1024)
    last = jnp.sum(small[4, :, 0:128], axis=1)
    return (grad, bias, term, last)


def solution(mesh):
    return jax.shard_map(
        on_device,
        mesh=mesh,
        in_specs=(
            P("batch", "seq", None),
            P("batch", "seq", None),
            P("batch", "seq", None),
            P("batch"),
            P("batch", None),
            P(),
            P(),
            P(),
            P(),
        ),
        out_specs=(P(("seq", "batch"), None), P(), P(), P()),
        check_vma=False,
    )
```

```python
import functools
import math

import jax
import jax.numpy as jnp
from jax import lax
from jax.experimental import pallas as pl
from jax.experimental.pallas import tpu as pltpu
from jax.sharding import PartitionSpec as P

MESH = pl.DeviceIdType.MESH
F32 = jnp.float32
BF16 = jnp.bfloat16
VM = pltpu.VMEM
CK = 512
WK = 512
KW = 2
FP = 4


def place():
    seq = lax.axis_index("seq")
    x = lax.axis_index("batch")
    y = seq // 8
    row = lax.rem(seq, 8)
    core = lax.rem(seq, 2)
    return seq, x, y, row, core


def greet(seq, x, y, row, core):
    bar = pltpu.get_barrier_semaphore()
    n = 0
    for k in range(1, 8):
        pl.semaphore_signal(
            bar, inc=1, device_id=(y * 8 + lax.rem(row + k, 8), x), device_id_type=MESH
        )
        n += 1
    for k in range(1, 4):
        pl.semaphore_signal(
            bar, inc=1, device_id=(lax.rem(y + k, 4) * 8 + row, x), device_id_type=MESH
        )
        n += 1
    for k in range(1, 8):
        pl.semaphore_signal(bar, inc=1, device_id=group_peer(seq, x, core, k), device_id_type=MESH)
        n += 1
    pl.semaphore_wait(bar, n)


def group_rank(x, core):
    return core * 4 + x


def group_peer(seq, x, core, k):
    j = lax.rem(group_rank(x, core) + k, 8)
    return (seq - core + j // 4, lax.rem(j, 4))


def remote(src, dst, ss, rs, dev):
    return pltpu.make_async_remote_copy(
        src_ref=src, dst_ref=dst, send_sem=ss, recv_sem=rs, device_id=dev, device_id_type=MESH
    )


def spread_kernel(
    q_hbm, k_hbm, v_hbm, w_hbm, b_in, wo, bo, qg, kg, ft_all, sp, act, pred, wot,
    q, k, v, ft, wbuf, pre, wsem, isem, ks, kr, qs, qr, fs, fr, ys, yr, ls,
):
    seq, x, y, row, core = place()
    j = group_rank(x, core)
    chunks = w_hbm.shape[0] // WK
    ins = [
        pltpu.make_async_copy(k_hbm, k, isem.at[0]),
        pltpu.make_async_copy(q_hbm, q, isem.at[1]),
        pltpu.make_async_copy(v_hbm, v, isem.at[2]),
    ]
    for c in ins:
        c.start()

    def fetch(i):
        return pltpu.make_async_copy(
            w_hbm.at[pl.ds(i * WK, WK)], wbuf.at[i % 3], wsem.at[i % 3]
        )

    fetch(0).start()
    fetch(1).start()
    greet(seq, x, y, row, core)
    kc, qc, fc, yc = [], [], [], []
    ins[0].wait()
    for n in range(1, 8):
        to = lax.rem(row + n, 8)
        c = remote(
            k.at[:, pl.ds(pl.multiple_of(to * 128, 128), 128)], kg.at[seq],
            ks.at[n], kr.at[n], (y * 8 + to, x),
        )
        c.start()
        kc.append(c)
    own_k = pltpu.make_async_copy(
        k.at[:, pl.ds(pl.multiple_of(row * 128, 128), 128)], kg.at[seq], ls.at[0]
    )
    own_k.start()
    ins[1].wait()
    for n in range(1, 8):
        to = lax.rem(row + n, 8)
        c = remote(
            q.at[:, pl.ds(pl.multiple_of(to * 512, 512), 512)], qg.at[row],
            qs.at[n], qr.at[n], (y * 8 + to, x),
        )
        c.start()
        qc.append(c)
    own_q = pltpu.make_async_copy(
        q.at[:, pl.ds(pl.multiple_of(row * 512, 512), 512)], qg.at[row], ls.at[1]
    )
    own_q.start()
    ins[2].wait()
    lanes = pl.ds(pl.multiple_of(j * 128, 128), 128)
    own_f = []
    for part in range(FP):
        span = 16 // FP
        for i in range(part * span, part * span + span):
            pieces = []
            for t in range(3):
                col = i * 384 + t * 128
                if col < 4096:
                    pieces.append(q[:, col : col + 128])
                elif col < 5120:
                    pieces.append(k[:, col - 4096 : col - 3968])
                else:
                    pieces.append(v[:, col - 5120 : col - 4992])
            block = jnp.concatenate(pieces, axis=1).astype(F32).T.astype(BF16)
            for t in range(8):
                ft[i, t] = block[t * 48 : (t + 1) * 48]
        some = pl.ds(part * span, span)
        for n in range(1, 8):
            to = lax.rem(j + n, 8)
            c = remote(
                ft.at[some, to], ft_all.at[some, :, lanes],
                fs.at[part * 8 + n], fr.at[part * 8 + n], group_peer(seq, x, core, n),
            )
            c.start()
            fc.append(c)
        c = pltpu.make_async_copy(ft.at[some, j], ft_all.at[some, :, lanes], ls.at[2 + part])
        c.start()
        own_f.append(c)

    def multiply(i):
        if i + 2 < chunks:
            fetch(i + 2).start()
        fetch(i).wait()
        lo = i * WK
        if lo < 4096:
            a = q[:, lo : lo + WK]
        elif lo < 5120:
            a = k[:, lo - 4096 : lo - 4096 + WK]
        else:
            a = v[:, lo - 5120 : lo - 5120 + WK]
        part = jnp.dot(a, wbuf[i % 3], preferred_element_type=F32)
        pre[...] = part if i == 0 else pre[...] + part

    def pass_on(n):
        block = kg.at[y * 8 + lax.rem(row + 8 - n, 8)]
        for m in range(1, 4):
            c = remote(
                block, block, ys.at[n * 4 + m], yr.at[n * 4 + m],
                (lax.rem(y + m, 4) * 8 + row, x),
            )
            c.start()
            yc.append(c)

    own_k.wait()
    pass_on(0)
    for i in range(KW):
        multiply(i)
    for n in range(1, 8):
        kc[n - 1].wait_recv()
        pass_on(n)
    for i in range(KW, chunks):
        multiply(i)
    z = pre[...] + b_in[...]
    sig = jax.nn.sigmoid(z)
    a = (z * sig).astype(BF16)
    act[...] = a
    sp[...] = sig * (1.0 + z * (1.0 - sig))
    turned = jnp.concatenate([wo[...], jnp.zeros((120, 1024), BF16)], axis=0)
    wot[...] = turned
    p8 = lax.dot_general(turned, a, (((1,), (1,)), ((), ())), preferred_element_type=F32)
    for g in range(8):
        pred[g : g + 1] = p8[g : g + 1] + bo[g]
    for c in qc + fc + yc:
        c.wait()
    for c in kc:
        c.wait_send()
    own_q.wait()
    for c in own_f:
        c.wait()


def spread(q, k, v, w, b_in, wo, bo):
    dma = pltpu.SemaphoreType.DMA
    vmem = pl.BlockSpec(memory_space=VM)
    hbm = pl.BlockSpec(memory_space=pltpu.HBM)
    return pl.pallas_call(
        spread_kernel,
        name="spread",
        out_shape=(
            jax.ShapeDtypeStruct((8, 128, 512), BF16),
            jax.ShapeDtypeStruct((32, 128, 128), BF16),
            jax.ShapeDtypeStruct((16, 48, 1024), BF16),
            jax.ShapeDtypeStruct((128, 1024), F32),
            jax.ShapeDtypeStruct((128, 1024), BF16),
            jax.ShapeDtypeStruct((8, 128), F32),
            jax.ShapeDtypeStruct((128, 1024), BF16),
        ),
        in_specs=[hbm, hbm, hbm, hbm, vmem, vmem, pl.BlockSpec(memory_space=pltpu.SMEM)],
        out_specs=(vmem,) * 7,
        scratch_shapes=[
            VM((128, 4096), BF16),
            VM((128, 1024), BF16),
            VM((128, 1024), BF16),
            VM((16, 8, 48, 128), BF16),
            VM((3, WK, 1024), BF16),
            VM((128, 1024), F32),
            dma((3,)), dma((3,)),
            dma((8,)), dma((8,)), dma((8,)), dma((8,)),
            dma((8 * FP,)), dma((8 * FP,)), dma((32,)), dma((32,)),
            dma((2 + FP,)),
        ],
        compiler_params=pltpu.CompilerParams(
            collective_id=0, has_side_effects=True, vmem_limit_bytes=40 * 2**20
        ),
    )(q, k, v, w, b_in, wo, bo)


def mass_kernel(meta, length, qg, kg, out, live, kpos, s_ref, acc):
    seq, _, y, _, _ = place()
    limit = length[0]
    first = y * 8
    here = lax.broadcasted_iota(jnp.int32, (1, 128), 1) + meta[seq] * 128
    live[...] = (here < limit).astype(F32)
    factor = math.log2(math.e) / math.sqrt(128)

    def order(r, _):
        kpos[pl.ds(pl.multiple_of(meta[r] * 128, 128), 128)] = kg[r]
        return 0

    lax.fori_loop(0, 32, order, 0)
    acc[...] = jnp.zeros_like(acc)
    lane = lax.rem(lax.broadcasted_iota(jnp.int32, (1, 512), 1), 128)
    sub = lax.broadcasted_iota(jnp.int32, (CK, 512), 0)

    def fold(a, op):
        return op(a.reshape(CK // 8, 8, 512), axis=0)

    def block(i, _):
        pos = meta[first + i]

        @pl.when(pos * 128 < limit)
        def _():
            last = pos * 128 // CK
            q4 = jnp.concatenate([qg[i, :, h * 128 : (h + 1) * 128] for h in range(4)], axis=0)

            def scores(c):
                rows = pl.ds(pl.multiple_of(c * CK, CK), CK)
                return rows, lax.dot_general(
                    kpos[rows], q4, (((1,), (1,)), ((), ())), preferred_element_type=F32
                )

            def first_pass(c, top):
                rows, s = scores(c)
                s_ref[rows] = s
                return jnp.maximum(top, fold(s, jnp.max))

            top = lax.fori_loop(0, last, first_pass, jnp.full((8, 512), -1e30, F32))
            rows, s = scores(last)
            s = jnp.where(sub + last * CK <= lane + pos * 128, s, -1e30)
            s_ref[rows] = s
            top = jnp.max(jnp.maximum(top, fold(s, jnp.max)), axis=0, keepdims=True)

            def second_pass(c, total):
                rows = pl.ds(pl.multiple_of(c * CK, CK), CK)
                e = jnp.exp2((s_ref[rows] - top) * factor)
                s_ref[rows] = e
                return total + fold(e, jnp.sum)

            total = lax.fori_loop(0, last + 1, second_pass, jnp.zeros((8, 512), F32))
            total = jnp.sum(total, axis=0, keepdims=True)
            share = jnp.where(lane + pos * 128 < limit, 1.0 / total, 0.0)

            def third_pass(c, _):
                rows = pl.ds(pl.multiple_of(c * CK, CK), CK)
                e = s_ref[rows] * share
                acc[rows] += (e[:, 0:128] + e[:, 128:256]) + (e[:, 256:384] + e[:, 384:512])
                return 0

            lax.fori_loop(0, last + 1, third_pass, 0)

        return 0

    lax.fori_loop(0, 8, block, 0)

    def give(r, _):
        rows = acc[pl.ds(pl.multiple_of(meta[r] * 128, 128), 128)]
        out[pl.ds(r, 1)] = jnp.sum(rows.T, axis=0, keepdims=True)
        return 0

    lax.fori_loop(0, 32, give, 0)


def column_mass(order, length, qg, kg):
    smem = pl.BlockSpec(memory_space=pltpu.SMEM)
    vmem = pl.BlockSpec(memory_space=VM)
    return pl.pallas_call(
        mass_kernel,
        name="column_mass",
        out_shape=(jax.ShapeDtypeStruct((32, 128), F32), jax.ShapeDtypeStruct((1, 128), F32)),
        in_specs=[smem, smem, vmem, vmem],
        out_specs=(vmem, vmem),
        scratch_shapes=[VM((4096, 128), BF16), VM((4096, 512), F32), VM((4096, 128), F32)],
        compiler_params=pltpu.CompilerParams(vmem_limit_bytes=40 * 2**20),
    )(order, length, qg, kg)


def reduce_kernel(
    norm, mass, sp, act, pred, live, wo, ft, out, small,
    m1, m2s, m2, dl, gs, res, rs, ps, ts, pk, p1, p2, p3,
    s1, r1, s2, r2, s3, r3, s4, r4, s5, r5, s6, r6, s7, r7, s8, r8, s9, r9,
):
    seq, x, y, row, core = place()
    z = row // 2
    j = group_rank(x, core)
    greet(seq, x, y, row, core)

    def y_dev(n):
        return (lax.rem(y + n, 4) * 8 + row, x)

    def z_dev(n):
        return (y * 8 + lax.rem(z + n, 4) * 2 + core, x)

    cs = []
    for n in range(1, 4):
        c = remote(mass.at[lax.rem(y + n, 4)], m1.at[y], s1.at[n], r1.at[n], y_dev(n))
        c.start()
        cs.append(c)
    m1[y] = mass[y]
    for c in cs:
        c.wait()
    total = (m1[0] + m1[1]) + (m1[2] + m1[3])
    for i in range(8):
        m2s[i] = jnp.broadcast_to(total[i : i + 1], (8, 128))
    cs = []
    for n in range(1, 8):
        to = lax.rem(row + n, 8)
        c = remote(m2s.at[to], m2.at[row], s2.at[n], r2.at[n], (y * 8 + to, x))
        c.start()
        cs.append(c)
    m2[row] = m2s[row]
    for c in cs:
        c.wait()
    label = jnp.concatenate([jnp.log1p(m2[i, 0:1]) for i in range(8)], axis=0)
    resid = ((pred[...] - label) * live[...] * norm).astype(BF16).astype(F32)
    wide = jnp.concatenate([resid, jnp.zeros((120, 128), F32)], axis=0)
    back = jnp.dot(wide.T.astype(BF16), wo[...], preferred_element_type=F32)
    delta = (back * sp[...]).astype(BF16)
    other = (seq + 1 - 2 * core, x)
    base = core * 4
    for p in range(4):
        dl[p, j] = delta[:, p * 256 : (p + 1) * 256]

    def give(p, slot, n, dev):
        return remote(dl.at[p, slot], dl.at[p, slot], s3.at[p * 8 + n], r3.at[p * 8 + n], dev)

    direct = [[give(p, j, n, (seq, lax.rem(x + n, 4))) for n in (2, 1, 3)] for p in range(4)]
    passed = [
        [give(p, base + lax.rem(x + 4 - n, 4), 4 + n, other) for n in (0, 2, 1, 3)]
        for p in range(4)
    ]
    for p in range(4):
        for c in direct[p]:
            c.start()
        passed[p][0].start()
    term = jnp.dot(wide.astype(BF16), act[...], preferred_element_type=F32)[0:8]
    bias = jnp.sum(delta.astype(F32), axis=0, keepdims=True)
    for i in range(4):
        pk[i] = term[:, i * 256 : (i + 1) * 256]
    pk[4, :, 0:128] = resid
    for i in range(8):
        pk[4, i : i + 1, 128:256] = bias[:, i * 128 : (i + 1) * 128]
    for i in range(5, 8):
        pk[i] = jnp.zeros((8, 256), F32)
    xs = []
    for n in range(1, 8):
        c = remote(
            pk.at[lax.rem(j + n, 8)], p1.at[j], s4.at[n], r4.at[n], group_peer(seq, x, core, n)
        )
        c.start()
        xs.append(c)
    p1[j] = pk[j]

    first, second = [], []

    def fold(h):
        for c in first[h]:
            c.wait()
        if h % 2 == 0:
            t = res[h, y]
            for n in range(1, 4):
                t = t + rs[h, lax.rem(y + n, 4)].astype(F32)
        else:
            t = res[h, :, z]
            for n in range(1, 4):
                t = t + rs[h, lax.rem(z + n, 4)].astype(F32)
        ps[h] = t
        cs = []
        for n in range(1, 4):
            if h % 2 == 0:
                c = remote(
                    ps.at[h, lax.rem(z + n, 4)], ts.at[h, z],
                    s9.at[h * 4 + n], r9.at[h * 4 + n], z_dev(n),
                )
            else:
                c = remote(
                    ps.at[h, lax.rem(y + n, 4)], ts.at[h, y],
                    s9.at[h * 4 + n], r9.at[h * 4 + n], y_dev(n),
                )
            c.start()
            cs.append(c)
        second.append(cs)

    f_all = ft[...].reshape(768, 1024)
    for p in range(4):
        for c, d in zip(direct[p], passed[p][1:]):
            c.wait_recv()
            d.start()
        for c in passed[p]:
            c.wait_recv()
        g = jnp.dot(f_all, dl[p].reshape(1024, 256), preferred_element_type=F32)
        for h in (2 * p, 2 * p + 1):
            half = g[:, (h % 2) * 128 : (h % 2) * 128 + 128].reshape(4, 4, 48, 128)
            gs[h] = half.astype(BF16)
            res[h] = half
            cs = []
            for n in range(1, 4):
                if h % 2 == 0:
                    c = remote(
                        gs.at[h, lax.rem(y + n, 4)], rs.at[h, y],
                        s8.at[h * 4 + n], r8.at[h * 4 + n], y_dev(n),
                    )
                else:
                    c = remote(
                        gs.at[h, :, lax.rem(z + n, 4)], rs.at[h, z],
                        s8.at[h * 4 + n], r8.at[h * 4 + n], z_dev(n),
                    )
                c.start()
                cs.append(c)
            first.append(cs)
        if p >= 1:
            fold(2 * p - 2)
            fold(2 * p - 1)
        if p == 1:
            for c in xs:
                c.wait()
            t = p1[0]
            for i in range(1, 8):
                t = t + p1[i]
            p2[y] = t
            ys = []
            for n in range(1, 4):
                c = remote(p2.at[y], p2.at[y], s5.at[n], r5.at[n], y_dev(n))
                c.start()
                ys.append(c)
        if p == 3:
            for c in ys:
                c.wait()
            p3[z] = (p2[0] + p2[1]) + (p2[2] + p2[3])
            zs = []
            for n in range(1, 4):
                c = remote(p3.at[z], p3.at[z], s6.at[n], r6.at[n], z_dev(n))
                c.start()
                zs.append(c)
    for p in range(4):
        for c in direct[p] + passed[p]:
            c.wait_send()
    fold(6)
    fold(7)
    for c in zs:
        c.wait()
    small[j] = (p3[0] + p3[1]) + (p3[2] + p3[3])
    fin = []
    for n in range(1, 8):
        c = remote(small.at[j], small.at[j], s7.at[n], r7.at[n], group_peer(seq, x, core, n))
        c.start()
        fin.append(c)
    for h in range(8):
        for c in second[h]:
            c.wait()
        if h % 2 == 0:
            t = ps[h, z]
            for n in range(1, 4):
                t = t + ts[h, lax.rem(z + n, 4)]
        else:
            t = ps[h, y]
            for n in range(1, 4):
                t = t + ts[h, lax.rem(y + n, 4)]
        out[:, h * 128 : (h + 1) * 128] = t
    for c in fin:
        c.wait()


def reduce_all(norm, mass, sp, act, pred, live, wo, ft):
    dma = pltpu.SemaphoreType.DMA
    vmem = pl.BlockSpec(memory_space=VM)
    return pl.pallas_call(
        functools.partial(reduce_kernel, norm),
        name="reduce_all",
        out_shape=(
            jax.ShapeDtypeStruct((48, 1024), F32),
            jax.ShapeDtypeStruct((8, 8, 256), F32),
        ),
        in_specs=[vmem] * 7,
        out_specs=(vmem,) * 2,
        scratch_shapes=[
            VM((4, 8, 128), F32), VM((8, 8, 128), F32), VM((8, 8, 128), F32),
            VM((4, 8, 128, 256), BF16),
            VM((8, 4, 4, 48, 128), BF16),
            VM((8, 4, 4, 48, 128), F32),
            VM((8, 4, 4, 48, 128), BF16),
            VM((8, 4, 48, 128), F32),
            VM((8, 4, 48, 128), F32),
            VM((8, 8, 256), F32), VM((8, 8, 256), F32), VM((4, 8, 256), F32), VM((4, 8, 256), F32),
        ]
        + [dma((4,)), dma((4,)), dma((8,)), dma((8,)), dma((32,)), dma((32,)), dma((8,)), dma((8,))]
        + [dma((4,)), dma((4,)), dma((4,)), dma((4,)), dma((8,)), dma((8,))]
        + [dma((32,)), dma((32,)), dma((32,)), dma((32,))],
        compiler_params=pltpu.CompilerParams(
            collective_id=1, has_side_effects=True, vmem_limit_bytes=40 * 2**20
        ),
    )(mass, sp, act, pred, live, wo, ft)


def finish_kernel(g, small, grad, bias, term, last):
    grad[...] = g[...]
    bias[...] = small[4, :, 128:256]
    t = jnp.concatenate([small[i] for i in range(4)], axis=1)
    term[...] = t
    r = jnp.concatenate([small[4, :, 0:128], jnp.zeros((120, 128), F32)], axis=0).T
    last[...] = jnp.sum(r, axis=0, keepdims=True)[:, 0:8]


def finish(g, small):
    vmem = pl.BlockSpec(memory_space=VM)
    return pl.pallas_call(
        finish_kernel,
        name="finish",
        out_shape=(
            jax.ShapeDtypeStruct((48, 1024), F32),
            jax.ShapeDtypeStruct((8, 128), F32),
            jax.ShapeDtypeStruct((8, 1024), F32),
            jax.ShapeDtypeStruct((1, 8), F32),
        ),
        in_specs=[vmem] * 2,
        out_specs=(vmem,) * 4,
    )(g, small)


def on_device(queries, keys, values, lengths, block_pos, w_in, b_in, output_weight, output_bias):
    norm = 1.0 / math.sqrt(4 * 4096)
    qg, kg, ft, sp, act, pred, wot = spread(
        queries[0], keys[0], values[0], w_in, b_in[None, :], output_weight.T, output_bias
    )
    mass, live = column_mass(block_pos[0], lengths, qg, kg)
    g, small = reduce_all(norm, mass.reshape(4, 8, 128), sp, act, pred, live, wot, ft)
    grad, bias, term, last = finish(g, small)
    return (grad, bias.reshape(1024), term.T, last.reshape(8))


def solution(mesh):
    return jax.shard_map(
        on_device,
        mesh=mesh,
        in_specs=(
            P("batch", "seq", None),
            P("batch", "seq", None),
            P("batch", "seq", None),
            P("batch"),
            P("batch", None),
            P(),
            P(),
            P(),
            P(),
        ),
        out_specs=(P(("seq", "batch"), None), P(), P(), P()),
        check_vma=False,
    )
```

```python
import functools
import math

import jax
import jax.numpy as jnp
from jax import lax
from jax.experimental import pallas as pl
from jax.experimental.pallas import tpu as pltpu
from jax.sharding import PartitionSpec as P

MESH = pl.DeviceIdType.MESH
F32 = jnp.float32
BF16 = jnp.bfloat16
VM = pltpu.VMEM
CK = 512
WK = 512
KW = 2
PARTS = ((0, 1), (2, 3), (4, 5), (6, 7))
EARLY = 3
FP = 4


def place():
    seq = lax.axis_index("seq")
    x = lax.axis_index("batch")
    y = seq // 8
    row = lax.rem(seq, 8)
    core = lax.rem(seq, 2)
    return seq, x, y, row, core


def greet(seq, x, y, row, core):
    bar = pltpu.get_barrier_semaphore()
    n = 0
    near = [(y * 8 + lax.rem(row + k, 8), x) for k in range(1, 8)]
    near += [(lax.rem(y + k, 4) * 8 + row, x) for k in range(1, 4)]
    for dev in near:
        pl.semaphore_signal(bar, inc=1, device_id=dev, device_id_type=MESH)
        n += 1
    for k in range(1, 8):
        pl.semaphore_signal(bar, inc=1, device_id=group_peer(seq, x, core, k), device_id_type=MESH)
        n += 1
    return functools.partial(pl.semaphore_wait, bar, n)


def group_rank(x, core):
    return core * 4 + x


def group_peer(seq, x, core, k):
    j = lax.rem(group_rank(x, core) + k, 8)
    return (seq - core + j // 4, lax.rem(j, 4))


def remote(src, dst, ss, rs, dev):
    return pltpu.make_async_remote_copy(
        src_ref=src, dst_ref=dst, send_sem=ss, recv_sem=rs, device_id=dev, device_id_type=MESH
    )


def spread_kernel(
    q_hbm, k_hbm, v_hbm, w_hbm, qg, kg, ft_all, pre,
    q, k, v, ft, wbuf, wsem, isem, ks, kr, qs, qr, fs, fr, ys, yr, ls,
):
    seq, x, y, row, core = place()
    j = group_rank(x, core)
    chunks = w_hbm.shape[0] // WK
    ins = [
        pltpu.make_async_copy(q_hbm, q, isem.at[0]),
        pltpu.make_async_copy(k_hbm, k, isem.at[1]),
        pltpu.make_async_copy(v_hbm, v, isem.at[2]),
    ]
    for c in ins:
        c.start()

    def fetch(i):
        return pltpu.make_async_copy(
            w_hbm.at[pl.ds(i * WK, WK)], wbuf.at[i % 3], wsem.at[i % 3]
        )

    fetch(0).start()
    fetch(1).start()
    met = greet(seq, x, y, row, core)
    for c in ins:
        c.wait()
    lanes = pl.ds(pl.multiple_of(j * 128, 128), 128)
    kc, qc, fc, yc, own_f = [], [], [], [], []
    span = 16 // FP

    def turn(part):
        for i in range(part * span, part * span + span):
            pieces = []
            for t in range(3):
                col = i * 384 + t * 128
                if col < 4096:
                    pieces.append(q[:, col : col + 128])
                elif col < 5120:
                    pieces.append(k[:, col - 4096 : col - 3968])
                else:
                    pieces.append(v[:, col - 5120 : col - 4992])
            block = jnp.concatenate(pieces, axis=1).astype(F32).T.astype(BF16)
            for t in range(8):
                ft[i, t] = block[t * 48 : (t + 1) * 48]

    def send(part):
        some = pl.ds(part * span, span)
        for n in (2, 6, 1, 3, 5, 7, 4):
            to = lax.rem(j + n, 8)
            c = remote(
                ft.at[some, to], ft_all.at[some, :, lanes],
                fs.at[part * 8 + n], fr.at[part * 8 + n], group_peer(seq, x, core, n),
            )
            c.start()
            fc.append(c)
        c = pltpu.make_async_copy(ft.at[some, j], ft_all.at[some, :, lanes], ls.at[2 + part])
        c.start()
        own_f.append(c)

    for part in range(EARLY):
        turn(part)
    met()
    for n in range(1, 8):
        to = lax.rem(row + n, 8)
        c = remote(
            k.at[:, pl.ds(pl.multiple_of(to * 128, 128), 128)], kg.at[seq],
            ks.at[n], kr.at[n], (y * 8 + to, x),
        )
        c.start()
        kc.append(c)
    own_k = pltpu.make_async_copy(
        k.at[:, pl.ds(pl.multiple_of(row * 128, 128), 128)], kg.at[seq], ls.at[0]
    )
    own_k.start()
    for part in range(EARLY):
        send(part)
    for n in range(1, 8):
        to = lax.rem(row + n, 8)
        c = remote(
            q.at[:, pl.ds(pl.multiple_of(to * 512, 512), 512)], qg.at[row],
            qs.at[n], qr.at[n], (y * 8 + to, x),
        )
        c.start()
        qc.append(c)
    own_q = pltpu.make_async_copy(
        q.at[:, pl.ds(pl.multiple_of(row * 512, 512), 512)], qg.at[row], ls.at[1]
    )
    own_q.start()
    for part in range(EARLY, FP):
        turn(part)
        send(part)

    def multiply(i):
        if i + 2 < chunks:
            fetch(i + 2).start()
        fetch(i).wait()
        lo = i * WK
        if lo < 4096:
            a = q[:, lo : lo + WK]
        elif lo < 5120:
            a = k[:, lo - 4096 : lo - 4096 + WK]
        else:
            a = v[:, lo - 5120 : lo - 5120 + WK]
        part = jnp.dot(a, wbuf[i % 3], preferred_element_type=F32)
        pre[...] = part if i == 0 else pre[...] + part

    def pass_on(n):
        block = kg.at[y * 8 + lax.rem(row + 8 - n, 8)]
        for m in range(1, 4):
            c = remote(
                block, block, ys.at[n * 4 + m], yr.at[n * 4 + m],
                (lax.rem(y + m, 4) * 8 + row, x),
            )
            c.start()
            yc.append(c)

    own_k.wait()
    pass_on(0)
    for i in range(KW):
        multiply(i)
    for n in range(1, 8):
        kc[n - 1].wait_recv()
        pass_on(n)
    for i in range(KW, chunks):
        multiply(i)
    for c in qc + fc + yc:
        c.wait()
    for c in kc:
        c.wait_send()
    own_q.wait()
    for c in own_f:
        c.wait()


def spread(q, k, v, w):
    dma = pltpu.SemaphoreType.DMA
    vmem = pl.BlockSpec(memory_space=VM)
    hbm = pl.BlockSpec(memory_space=pltpu.HBM)
    return pl.pallas_call(
        spread_kernel,
        name="spread",
        out_shape=(
            jax.ShapeDtypeStruct((8, 128, 512), BF16),
            jax.ShapeDtypeStruct((32, 128, 128), BF16),
            jax.ShapeDtypeStruct((16, 48, 1024), BF16),
            jax.ShapeDtypeStruct((128, 1024), F32),
        ),
        in_specs=[hbm, hbm, hbm, hbm],
        out_specs=(vmem,) * 4,
        scratch_shapes=[
            VM((128, 4096), BF16),
            VM((128, 1024), BF16),
            VM((128, 1024), BF16),
            VM((16, 8, 48, 128), BF16),
            VM((3, WK, 1024), BF16),
            dma((3,)), dma((3,)),
            dma((8,)), dma((8,)), dma((8,)), dma((8,)),
            dma((8 * FP,)), dma((8 * FP,)), dma((32,)), dma((32,)),
            dma((2 + FP,)),
        ],
        compiler_params=pltpu.CompilerParams(
            collective_id=0, has_side_effects=True, vmem_limit_bytes=40 * 2**20
        ),
    )(q, k, v, w)


def mass_kernel(meta, length, qg, kg, out, live, kpos, s_ref, acc):
    seq, _, y, _, _ = place()
    limit = length[0]
    first = y * 8
    here = lax.broadcasted_iota(jnp.int32, (1, 128), 1) + meta[seq] * 128
    live[...] = (here < limit).astype(F32)
    factor = math.log2(math.e) / math.sqrt(128)

    def order(r, _):
        kpos[pl.ds(pl.multiple_of(meta[r] * 128, 128), 128)] = kg[r]
        return 0

    lax.fori_loop(0, 32, order, 0)
    acc[...] = jnp.zeros_like(acc)
    lane = lax.rem(lax.broadcasted_iota(jnp.int32, (1, 512), 1), 128)
    sub = lax.broadcasted_iota(jnp.int32, (CK, 512), 0)

    def fold(a, op):
        return op(a.reshape(CK // 8, 8, 512), axis=0)

    def block(i, _):
        pos = meta[first + i]

        @pl.when(pos * 128 < limit)
        def _():
            last = pos * 128 // CK
            q4 = jnp.concatenate([qg[i, :, h * 128 : (h + 1) * 128] for h in range(4)], axis=0)

            def scores(c):
                rows = pl.ds(pl.multiple_of(c * CK, CK), CK)
                return rows, lax.dot_general(
                    kpos[rows], q4, (((1,), (1,)), ((), ())), preferred_element_type=F32
                )

            def first_pass(c, top):
                rows, s = scores(c)
                s_ref[rows] = s
                return jnp.maximum(top, fold(s, jnp.max))

            top = lax.fori_loop(0, last, first_pass, jnp.full((8, 512), -1e30, F32))
            rows, s = scores(last)
            s = jnp.where(sub + last * CK <= lane + pos * 128, s, -1e30)
            s_ref[rows] = s
            top = jnp.max(jnp.maximum(top, fold(s, jnp.max)), axis=0, keepdims=True)

            def second_pass(c, total):
                rows = pl.ds(pl.multiple_of(c * CK, CK), CK)
                e = jnp.exp2((s_ref[rows] - top) * factor)
                s_ref[rows] = e
                return total + fold(e, jnp.sum)

            total = lax.fori_loop(0, last + 1, second_pass, jnp.zeros((8, 512), F32))
            total = jnp.sum(total, axis=0, keepdims=True)
            share = jnp.where(lane + pos * 128 < limit, 1.0 / total, 0.0)

            def third_pass(c, _):
                rows = pl.ds(pl.multiple_of(c * CK, CK), CK)
                e = s_ref[rows] * share
                acc[rows] += (e[:, 0:128] + e[:, 128:256]) + (e[:, 256:384] + e[:, 384:512])
                return 0

            lax.fori_loop(0, last + 1, third_pass, 0)

        return 0

    lax.fori_loop(0, 8, block, 0)

    def give(r, _):
        rows = acc[pl.ds(pl.multiple_of(meta[r] * 128, 128), 128)]
        out[pl.ds(r, 1)] = jnp.sum(rows.T, axis=0, keepdims=True)
        return 0

    lax.fori_loop(0, 32, give, 0)


def column_mass(order, length, qg, kg):
    smem = pl.BlockSpec(memory_space=pltpu.SMEM)
    vmem = pl.BlockSpec(memory_space=VM)
    return pl.pallas_call(
        mass_kernel,
        name="column_mass",
        out_shape=(jax.ShapeDtypeStruct((32, 128), F32), jax.ShapeDtypeStruct((1, 128), F32)),
        in_specs=[smem, smem, vmem, vmem],
        out_specs=(vmem, vmem),
        scratch_shapes=[VM((4096, 128), BF16), VM((4096, 512), F32), VM((4096, 128), F32)],
        compiler_params=pltpu.CompilerParams(vmem_limit_bytes=40 * 2**20),
    )(order, length, qg, kg)


def reduce_kernel(
    norm, mass, pre, b_in, wo, bo, live, ft, out, small,
    m1, m2s, m2, dl, gs, res, rs, ps, ts, pk, p1, p2, p3,
    s1, r1, s2, r2, s3, r3, s4, r4, s5, r5, s6, r6, s7, r7, s8, r8, s9, r9,
):
    seq, x, y, row, core = place()
    z = row // 2
    j = group_rank(x, core)
    greet(seq, x, y, row, core)()

    def y_dev(n):
        return (lax.rem(y + n, 4) * 8 + row, x)

    def z_dev(n):
        return (y * 8 + lax.rem(z + n, 4) * 2 + core, x)

    cs = []
    for n in range(1, 4):
        c = remote(mass.at[lax.rem(y + n, 4)], m1.at[y], s1.at[n], r1.at[n], y_dev(n))
        c.start()
        cs.append(c)
    m1[y] = mass[y]
    lin = pre[...] + b_in[...]
    sig = jax.nn.sigmoid(lin)
    act = (lin * sig).astype(BF16)
    slope = sig * (1.0 + lin * (1.0 - sig))
    wide_o = jnp.concatenate([wo[...], jnp.zeros((120, 1024), BF16)], axis=0)
    for c in cs:
        c.wait()
    total = (m1[0] + m1[1]) + (m1[2] + m1[3])
    for i in range(8):
        m2s[i] = jnp.broadcast_to(total[i : i + 1], (8, 128))
    cs = []
    for n in range(1, 8):
        to = lax.rem(row + n, 8)
        c = remote(m2s.at[to], m2.at[row], s2.at[n], r2.at[n], (y * 8 + to, x))
        c.start()
        cs.append(c)
    m2[row] = m2s[row]
    p8 = lax.dot_general(wide_o, act, (((1,), (1,)), ((), ())), preferred_element_type=F32)
    pred = jnp.concatenate([p8[g : g + 1] + bo[g] for g in range(8)], axis=0)
    for c in cs:
        c.wait()
    mass_t = jnp.concatenate([m2[g, 0:1] for g in range(8)], axis=0)
    label = jnp.log1p(mass_t)
    resid = ((pred - label) * live[...] * norm).astype(BF16).astype(F32)
    wide = jnp.concatenate([resid, jnp.zeros((120, 128), F32)], axis=0)
    back = jnp.dot(wide.T.astype(BF16), wide_o, preferred_element_type=F32)
    delta = (back * slope).astype(BF16)
    other = (seq + 1 - 2 * core, x)
    base = core * 4
    for h in range(8):
        dl[h, j] = delta[:, h * 128 : (h + 1) * 128]
    parts = len(PARTS)

    def give(p, slot, n, dev):
        some = dl.at[pl.ds(PARTS[p][0], len(PARTS[p])), slot]
        return remote(some, some, s3.at[p * 8 + n], r3.at[p * 8 + n], dev)

    direct = [[give(p, j, n, (seq, lax.rem(x + n, 4))) for n in (2, 1, 3)] for p in range(parts)]
    passed = [
        [give(p, base + lax.rem(x + 4 - n, 4), 4 + n, other) for n in (0, 2, 1, 3)]
        for p in range(parts)
    ]

    def set_out(p):
        for c in direct[p]:
            c.start()
        passed[p][0].start()

    set_out(0)
    term = jnp.dot(wide.astype(BF16), act, preferred_element_type=F32)[0:8]
    bias = jnp.sum(delta.astype(F32), axis=0, keepdims=True)
    for i in range(4):
        pk[i] = term[:, i * 256 : (i + 1) * 256]
    pk[4, :, 0:128] = resid
    for i in range(8):
        pk[4, i : i + 1, 128:256] = bias[:, i * 128 : (i + 1) * 128]
    for i in range(5, 8):
        pk[i] = jnp.zeros((8, 256), F32)
    xs = []
    for n in range(1, 8):
        c = remote(
            pk.at[lax.rem(j + n, 8)], p1.at[j], s4.at[n], r4.at[n], group_peer(seq, x, core, n)
        )
        c.start()
        xs.append(c)
    p1[j] = pk[j]
    for p in range(1, parts):
        set_out(p)

    first, second = [], []

    def fold(h):
        for c in first[h]:
            c.wait()
        if h % 2 == 0:
            t = res[h, y]
            for n in range(1, 4):
                t = t + rs[h, lax.rem(y + n, 4)].astype(F32)
        else:
            t = res[h, :, z]
            for n in range(1, 4):
                t = t + rs[h, lax.rem(z + n, 4)].astype(F32)
        ps[h] = t
        cs = []
        for n in range(1, 4):
            if h % 2 == 0:
                c = remote(
                    ps.at[h, lax.rem(z + n, 4)], ts.at[h, z],
                    s9.at[h * 4 + n], r9.at[h * 4 + n], z_dev(n),
                )
            else:
                c = remote(
                    ps.at[h, lax.rem(y + n, 4)], ts.at[h, y],
                    s9.at[h * 4 + n], r9.at[h * 4 + n], y_dev(n),
                )
            c.start()
            cs.append(c)
        second.append(cs)

    f_all = ft[...].reshape(768, 1024)
    for p in range(parts):
        for c, d in zip(direct[p], passed[p][1:]):
            c.wait_recv()
            d.start()
        for c in passed[p]:
            c.wait_recv()
        d_all = jnp.concatenate([dl[h].reshape(1024, 128) for h in PARTS[p]], axis=1)
        g = jnp.dot(f_all, d_all, preferred_element_type=F32)
        for i, h in enumerate(PARTS[p]):
            half = g[:, i * 128 : (i + 1) * 128].reshape(4, 4, 48, 128)
            gs[h] = half.astype(BF16)
            res[h] = half
            cs = []
            for n in range(1, 4):
                if h % 2 == 0:
                    c = remote(
                        gs.at[h, lax.rem(y + n, 4)], rs.at[h, y],
                        s8.at[h * 4 + n], r8.at[h * 4 + n], y_dev(n),
                    )
                else:
                    c = remote(
                        gs.at[h, :, lax.rem(z + n, 4)], rs.at[h, z],
                        s8.at[h * 4 + n], r8.at[h * 4 + n], z_dev(n),
                    )
                c.start()
                cs.append(c)
            first.append(cs)
        if p == 0:
            for c in xs:
                c.wait()
            t = p1[0]
            for i in range(1, 8):
                t = t + p1[i]
            p2[y] = t
            sy = []
            for n in range(1, 4):
                c = remote(p2.at[y], p2.at[y], s5.at[n], r5.at[n], y_dev(n))
                c.start()
                sy.append(c)
        if p >= 2:
            for h in PARTS[p - 2]:
                fold(h)
        if p == 2:
            for c in sy:
                c.wait()
            p3[z] = (p2[0] + p2[1]) + (p2[2] + p2[3])
            zs = []
            for n in range(1, 4):
                c = remote(p3.at[z], p3.at[z], s6.at[n], r6.at[n], z_dev(n))
                c.start()
                zs.append(c)
        if p == 3:
            for c in zs:
                c.wait()
            small[j] = (p3[0] + p3[1]) + (p3[2] + p3[3])
            fin = []
            for n in range(1, 8):
                c = remote(
                    small.at[j], small.at[j], s7.at[n], r7.at[n], group_peer(seq, x, core, n)
                )
                c.start()
                fin.append(c)
    for h in PARTS[parts - 2] + PARTS[parts - 1]:
        fold(h)
    for p in range(parts):
        for c in direct[p] + passed[p]:
            c.wait_send()
    for h in range(8):
        for c in second[h]:
            c.wait()
        if h % 2 == 0:
            t = ps[h, z]
            for n in range(1, 4):
                t = t + ts[h, lax.rem(z + n, 4)]
        else:
            t = ps[h, y]
            for n in range(1, 4):
                t = t + ts[h, lax.rem(y + n, 4)]
        out[:, h * 128 : (h + 1) * 128] = t
    for c in fin:
        c.wait()


def reduce_all(norm, mass, pre, b_in, wo, bo, live, ft):
    dma = pltpu.SemaphoreType.DMA
    vmem = pl.BlockSpec(memory_space=VM)
    smem = pl.BlockSpec(memory_space=pltpu.SMEM)
    return pl.pallas_call(
        functools.partial(reduce_kernel, norm),
        name="reduce_all",
        out_shape=(
            jax.ShapeDtypeStruct((48, 1024), F32),
            jax.ShapeDtypeStruct((8, 8, 256), F32),
        ),
        in_specs=[vmem, vmem, vmem, vmem, smem, vmem, vmem],
        out_specs=(vmem,) * 2,
        scratch_shapes=[
            VM((4, 8, 128), F32), VM((8, 8, 128), F32), VM((8, 8, 128), F32),
            VM((8, 8, 128, 128), BF16),
            VM((8, 4, 4, 48, 128), BF16),
            VM((8, 4, 4, 48, 128), F32),
            VM((8, 4, 4, 48, 128), BF16),
            VM((8, 4, 48, 128), F32),
            VM((8, 4, 48, 128), F32),
            VM((8, 8, 256), F32), VM((8, 8, 256), F32), VM((4, 8, 256), F32), VM((4, 8, 256), F32),
        ]
        + [dma((4,)), dma((4,)), dma((8,)), dma((8,)), dma((40,)), dma((40,)), dma((8,)), dma((8,))]
        + [dma((4,)), dma((4,)), dma((4,)), dma((4,)), dma((8,)), dma((8,))]
        + [dma((32,)), dma((32,)), dma((32,)), dma((32,))],
        compiler_params=pltpu.CompilerParams(
            collective_id=1, has_side_effects=True, vmem_limit_bytes=40 * 2**20
        ),
    )(mass, pre, b_in, wo, bo, live, ft)


def finish_kernel(g, small, grad, bias, term, last):
    grad[...] = g[...]
    bias[...] = small[4, :, 128:256]
    t = jnp.concatenate([small[i] for i in range(4)], axis=1)
    term[...] = t
    r = jnp.concatenate([small[4, :, 0:128], jnp.zeros((120, 128), F32)], axis=0).T
    last[...] = jnp.sum(r, axis=0, keepdims=True)[:, 0:8]


def finish(g, small):
    vmem = pl.BlockSpec(memory_space=VM)
    return pl.pallas_call(
        finish_kernel,
        name="finish",
        out_shape=(
            jax.ShapeDtypeStruct((48, 1024), F32),
            jax.ShapeDtypeStruct((8, 128), F32),
            jax.ShapeDtypeStruct((8, 1024), F32),
            jax.ShapeDtypeStruct((1, 8), F32),
        ),
        in_specs=[vmem] * 2,
        out_specs=(vmem,) * 4,
    )(g, small)


def on_device(queries, keys, values, lengths, block_pos, w_in, b_in, output_weight, output_bias):
    norm = 1.0 / math.sqrt(4 * 4096)
    qg, kg, ft, pre = spread(queries[0], keys[0], values[0], w_in)
    mass, live = column_mass(block_pos[0], lengths, qg, kg)
    g, small = reduce_all(
        norm, mass.reshape(4, 8, 128), pre, b_in[None, :], output_weight.T, output_bias, live, ft
    )
    grad, bias, term, last = finish(g, small)
    return (grad, bias.reshape(1024), term.T, last.reshape(8))


def solution(mesh):
    return jax.shard_map(
        on_device,
        mesh=mesh,
        in_specs=(
            P("batch", "seq", None),
            P("batch", "seq", None),
            P("batch", "seq", None),
            P("batch"),
            P("batch", None),
            P(),
            P(),
            P(),
            P(),
        ),
        out_specs=(P(("seq", "batch"), None), P(), P(), P()),
        check_vma=False,
    )
```

```python
import functools
import math

import jax
import jax.numpy as jnp
from jax import lax
from jax.experimental import pallas as pl
from jax.experimental.pallas import tpu as pltpu
from jax.sharding import PartitionSpec as P

MESH = pl.DeviceIdType.MESH
F32 = jnp.float32
BF16 = jnp.bfloat16
VM = pltpu.VMEM
CK = 512
WK = 512
KW = 2
PARTS = ((0, 1), (2, 3), (4, 5), (6, 7))
EARLY = 1
FP = 1


def place():
    seq = lax.axis_index("seq")
    x = lax.axis_index("batch")
    y = seq // 8
    row = lax.rem(seq, 8)
    core = lax.rem(seq, 2)
    return seq, x, y, row, core


def greet(seq, x, y, row, core):
    bar = pltpu.get_barrier_semaphore()
    n = 0
    near = [(y * 8 + lax.rem(row + k, 8), x) for k in range(1, 8)]
    near += [(lax.rem(y + k, 4) * 8 + row, x) for k in range(1, 4)]
    for dev in near:
        pl.semaphore_signal(bar, inc=1, device_id=dev, device_id_type=MESH)
        n += 1
    for k in range(1, 8):
        pl.semaphore_signal(bar, inc=1, device_id=group_peer(seq, x, core, k), device_id_type=MESH)
        n += 1
    return functools.partial(pl.semaphore_wait, bar, n)


def group_rank(x, core):
    return core * 4 + x


def group_peer(seq, x, core, k):
    j = lax.rem(group_rank(x, core) + k, 8)
    return (seq - core + j // 4, lax.rem(j, 4))


def remote(src, dst, ss, rs, dev):
    return pltpu.make_async_remote_copy(
        src_ref=src, dst_ref=dst, send_sem=ss, recv_sem=rs, device_id=dev, device_id_type=MESH
    )


def spread_kernel(
    q, k, v, w_hbm, qg, kg, ft_all, pre,
    ft, wbuf, wsem, ks, kr, qs, qr, fs, fr, ys, yr, ls,
):
    seq, x, y, row, core = place()
    j = group_rank(x, core)
    chunks = w_hbm.shape[0] // WK

    def fetch(i):
        return pltpu.make_async_copy(
            w_hbm.at[pl.ds(i * WK, WK)], wbuf.at[i % 3], wsem.at[i % 3]
        )

    fetch(0).start()
    fetch(1).start()
    met = greet(seq, x, y, row, core)
    lanes = pl.ds(pl.multiple_of(j * 128, 128), 128)
    kc, qc, fc, yc, own_f = [], [], [], [], []
    span = 16 // FP

    def turn(part):
        for i in range(part * span, part * span + span):
            pieces = []
            for t in range(3):
                col = i * 384 + t * 128
                if col < 4096:
                    pieces.append(q[:, col : col + 128])
                elif col < 5120:
                    pieces.append(k[:, col - 4096 : col - 3968])
                else:
                    pieces.append(v[:, col - 5120 : col - 4992])
            block = jnp.concatenate(pieces, axis=1).astype(F32).T.astype(BF16)
            for t in range(8):
                ft[i, t] = block[t * 48 : (t + 1) * 48]

    def send(part):
        some = pl.ds(part * span, span)
        for n in (2, 6, 1, 3, 5, 7, 4):
            to = lax.rem(j + n, 8)
            c = remote(
                ft.at[some, to], ft_all.at[some, :, lanes],
                fs.at[part * 8 + n], fr.at[part * 8 + n], group_peer(seq, x, core, n),
            )
            c.start()
            fc.append(c)
        c = pltpu.make_async_copy(ft.at[some, j], ft_all.at[some, :, lanes], ls.at[2 + part])
        c.start()
        own_f.append(c)

    for part in range(EARLY):
        turn(part)
    met()
    for n in range(4):
        cs = []
        for flip in range(2):
            if n == 0 and flip == 0:
                continue
            to = lax.rem(row // 2 + n, 4) * 2 + lax.rem(core + flip, 2)
            c = remote(
                k.at[:, pl.ds(pl.multiple_of(to * 128, 128), 128)], kg.at[seq],
                ks.at[n * 2 + flip], kr.at[n * 2 + flip], (y * 8 + to, x),
            )
            c.start()
            cs.append(c)
        kc.append(cs)
    own_k = pltpu.make_async_copy(
        k.at[:, pl.ds(pl.multiple_of(row * 128, 128), 128)], kg.at[seq], ls.at[0]
    )
    own_k.start()
    for part in range(EARLY):
        send(part)
    for n in range(1, 8):
        to = lax.rem(row + n, 8)
        c = remote(
            q.at[:, pl.ds(pl.multiple_of(to * 512, 512), 512)], qg.at[row],
            qs.at[n], qr.at[n], (y * 8 + to, x),
        )
        c.start()
        qc.append(c)
    own_q = pltpu.make_async_copy(
        q.at[:, pl.ds(pl.multiple_of(row * 512, 512), 512)], qg.at[row], ls.at[1]
    )
    own_q.start()
    for part in range(EARLY, FP):
        turn(part)
        send(part)

    def multiply(i):
        if i + 2 < chunks:
            fetch(i + 2).start()
        fetch(i).wait()
        lo = i * WK
        if lo < 4096:
            a = q[:, lo : lo + WK]
        elif lo < 5120:
            a = k[:, lo - 4096 : lo - 4096 + WK]
        else:
            a = v[:, lo - 5120 : lo - 5120 + WK]
        part = jnp.dot(a, wbuf[i % 3], preferred_element_type=F32)
        pre[...] = part if i == 0 else pre[...] + part

    def pass_on(n):
        pair = kg.at[pl.ds(y * 8 + lax.rem(row // 2 + 4 - n, 4) * 2, 2)]
        for m in (2, 1, 3):
            c = remote(
                pair, pair, ys.at[n * 4 + m], yr.at[n * 4 + m],
                (lax.rem(y + m, 4) * 8 + row, x),
            )
            c.start()
            yc.append(c)

    own_k.wait()
    for n in range(4):
        for c in kc[n]:
            c.wait_recv()
        pass_on(n)
        if n < KW:
            multiply(n)
    for i in range(KW, chunks):
        multiply(i)
    for c in qc + fc + yc:
        c.wait()
    for cs in kc:
        for c in cs:
            c.wait_send()
    own_q.wait()
    for c in own_f:
        c.wait()


def spread(q, k, v, w):
    dma = pltpu.SemaphoreType.DMA
    vmem = pl.BlockSpec(memory_space=VM)
    hbm = pl.BlockSpec(memory_space=pltpu.HBM)
    return pl.pallas_call(
        spread_kernel,
        name="spread",
        out_shape=(
            jax.ShapeDtypeStruct((8, 128, 512), BF16),
            jax.ShapeDtypeStruct((32, 128, 128), BF16),
            jax.ShapeDtypeStruct((16, 48, 1024), BF16),
            jax.ShapeDtypeStruct((128, 1024), F32),
        ),
        in_specs=[vmem, vmem, vmem, hbm],
        out_specs=(vmem,) * 4,
        scratch_shapes=[
            VM((16, 8, 48, 128), BF16),
            VM((3, WK, 1024), BF16),
            dma((3,)),
            dma((8,)), dma((8,)), dma((8,)), dma((8,)),
            dma((8 * FP,)), dma((8 * FP,)), dma((16,)), dma((16,)),
            dma((2 + FP,)),
        ],
        compiler_params=pltpu.CompilerParams(
            collective_id=0, has_side_effects=True, vmem_limit_bytes=40 * 2**20
        ),
    )(q, k, v, w)


def mass_kernel(meta, length, qg, kg, out, live, kpos, s_ref, acc):
    seq, _, y, _, _ = place()
    limit = length[0]
    first = y * 8
    here = lax.broadcasted_iota(jnp.int32, (1, 128), 1) + meta[seq] * 128
    live[...] = (here < limit).astype(F32)
    factor = math.log2(math.e) / math.sqrt(128)

    def order(r, _):
        kpos[pl.ds(pl.multiple_of(meta[r] * 128, 128), 128)] = kg[r]
        return 0

    lax.fori_loop(0, 32, order, 0)
    acc[...] = jnp.zeros_like(acc)
    lane = lax.rem(lax.broadcasted_iota(jnp.int32, (1, 512), 1), 128)
    sub = lax.broadcasted_iota(jnp.int32, (CK, 512), 0)

    def fold(a, op):
        return op(a.reshape(CK // 8, 8, 512), axis=0)

    def block(i, _):
        pos = meta[first + i]

        @pl.when(pos * 128 < limit)
        def _():
            last = pos * 128 // CK
            q4 = jnp.concatenate([qg[i, :, h * 128 : (h + 1) * 128] for h in range(4)], axis=0)

            def scores(c):
                rows = pl.ds(pl.multiple_of(c * CK, CK), CK)
                return rows, lax.dot_general(
                    kpos[rows], q4, (((1,), (1,)), ((), ())), preferred_element_type=F32
                )

            def first_pass(c, top):
                rows, s = scores(c)
                s_ref[rows] = s
                return jnp.maximum(top, fold(s, jnp.max))

            top = lax.fori_loop(0, last, first_pass, jnp.full((8, 512), -1e30, F32))
            rows, s = scores(last)
            s = jnp.where(sub + last * CK <= lane + pos * 128, s, -1e30)
            s_ref[rows] = s
            top = jnp.max(jnp.maximum(top, fold(s, jnp.max)), axis=0, keepdims=True)

            def second_pass(c, total):
                rows = pl.ds(pl.multiple_of(c * CK, CK), CK)
                e = jnp.exp2((s_ref[rows] - top) * factor)
                s_ref[rows] = e
                return total + fold(e, jnp.sum)

            total = lax.fori_loop(0, last + 1, second_pass, jnp.zeros((8, 512), F32))
            total = jnp.sum(total, axis=0, keepdims=True)
            share = jnp.where(lane + pos * 128 < limit, 1.0 / total, 0.0)

            def third_pass(c, _):
                rows = pl.ds(pl.multiple_of(c * CK, CK), CK)
                e = s_ref[rows] * share
                acc[rows] += (e[:, 0:128] + e[:, 128:256]) + (e[:, 256:384] + e[:, 384:512])
                return 0

            lax.fori_loop(0, last + 1, third_pass, 0)

        return 0

    lax.fori_loop(0, 8, block, 0)

    def give(r, _):
        rows = acc[pl.ds(pl.multiple_of(meta[r] * 128, 128), 128)]
        out[pl.ds(r, 1)] = jnp.sum(rows.T, axis=0, keepdims=True)
        return 0

    lax.fori_loop(0, 32, give, 0)


def column_mass(order, length, qg, kg):
    smem = pl.BlockSpec(memory_space=pltpu.SMEM)
    vmem = pl.BlockSpec(memory_space=VM)
    return pl.pallas_call(
        mass_kernel,
        name="column_mass",
        out_shape=(jax.ShapeDtypeStruct((32, 128), F32), jax.ShapeDtypeStruct((1, 128), F32)),
        in_specs=[smem, smem, vmem, vmem],
        out_specs=(vmem, vmem),
        scratch_shapes=[VM((4096, 128), BF16), VM((4096, 512), F32), VM((4096, 128), F32)],
        compiler_params=pltpu.CompilerParams(vmem_limit_bytes=40 * 2**20),
    )(order, length, qg, kg)


def reduce_kernel(
    norm, mass, pre, b_in, wo, bo, live, ft, out, small,
    m1, m2s, m2, dl, gs, res, rs, ps, ts, pk, p1, p2, p3,
    s1, r1, s2, r2, s3, r3, s4, r4, s5, r5, s6, r6, s7, r7, s8, r8, s9, r9,
):
    seq, x, y, row, core = place()
    z = row // 2
    j = group_rank(x, core)
    greet(seq, x, y, row, core)()

    def y_dev(n):
        return (lax.rem(y + n, 4) * 8 + row, x)

    def z_dev(n):
        return (y * 8 + lax.rem(z + n, 4) * 2 + core, x)

    cs = []
    for n in range(1, 4):
        c = remote(mass.at[lax.rem(y + n, 4)], m1.at[y], s1.at[n], r1.at[n], y_dev(n))
        c.start()
        cs.append(c)
    m1[y] = mass[y]
    lin = pre[...] + b_in[...]
    sig = jax.nn.sigmoid(lin)
    act = (lin * sig).astype(BF16)
    slope = sig * (1.0 + lin * (1.0 - sig))
    wide_o = jnp.concatenate([wo[...], jnp.zeros((120, 1024), BF16)], axis=0)
    for c in cs:
        c.wait()
    total = (m1[0] + m1[1]) + (m1[2] + m1[3])
    for i in range(8):
        m2s[i] = jnp.broadcast_to(total[i : i + 1], (8, 128))
    cs = []
    for n in range(1, 8):
        to = lax.rem(row + n, 8)
        c = remote(m2s.at[to], m2.at[row], s2.at[n], r2.at[n], (y * 8 + to, x))
        c.start()
        cs.append(c)
    m2[row] = m2s[row]
    p8 = lax.dot_general(wide_o, act, (((1,), (1,)), ((), ())), preferred_element_type=F32)
    pred = jnp.concatenate([p8[g : g + 1] + bo[g] for g in range(8)], axis=0)
    for c in cs:
        c.wait()
    mass_t = jnp.concatenate([m2[g, 0:1] for g in range(8)], axis=0)
    label = jnp.log1p(mass_t)
    resid = ((pred - label) * live[...] * norm).astype(BF16).astype(F32)
    wide = jnp.concatenate([resid, jnp.zeros((120, 128), F32)], axis=0)
    back = jnp.dot(wide.T.astype(BF16), wide_o, preferred_element_type=F32)
    delta = (back * slope).astype(BF16)
    other = (seq + 1 - 2 * core, x)
    base = core * 4
    for h in range(8):
        dl[h, j] = delta[:, h * 128 : (h + 1) * 128]
    parts = len(PARTS)

    def give(p, slot, n, dev):
        some = dl.at[pl.ds(PARTS[p][0], len(PARTS[p])), slot]
        return remote(some, some, s3.at[p * 8 + n], r3.at[p * 8 + n], dev)

    direct = [[give(p, j, n, (seq, lax.rem(x + n, 4))) for n in (2, 1, 3)] for p in range(parts)]
    passed = [
        [give(p, base + lax.rem(x + 4 - n, 4), 4 + n, other) for n in (0, 2, 1, 3)]
        for p in range(parts)
    ]

    def set_out(p):
        for c in direct[p]:
            c.start()
        passed[p][0].start()

    set_out(0)
    term = jnp.dot(wide.astype(BF16), act, preferred_element_type=F32)[0:8]
    bias = jnp.sum(delta.astype(F32), axis=0, keepdims=True)
    for i in range(4):
        pk[i] = term[:, i * 256 : (i + 1) * 256]
    pk[4, :, 0:128] = resid
    for i in range(8):
        pk[4, i : i + 1, 128:256] = bias[:, i * 128 : (i + 1) * 128]
    for i in range(5, 8):
        pk[i] = jnp.zeros((8, 256), F32)
    xs = []
    for n in range(1, 8):
        c = remote(
            pk.at[lax.rem(j + n, 8)], p1.at[j], s4.at[n], r4.at[n], group_peer(seq, x, core, n)
        )
        c.start()
        xs.append(c)
    p1[j] = pk[j]
    for p in range(1, parts):
        set_out(p)

    first, second = [], []

    def fold(h):
        for c in first[h]:
            c.wait()
        if h % 2 == 0:
            t = res[h, y]
            for n in range(1, 4):
                t = t + rs[h, lax.rem(y + n, 4)].astype(F32)
        else:
            t = res[h, :, z]
            for n in range(1, 4):
                t = t + rs[h, lax.rem(z + n, 4)].astype(F32)
        ps[h] = t
        cs = []
        for n in range(1, 4):
            if h % 2 == 0:
                c = remote(
                    ps.at[h, lax.rem(z + n, 4)], ts.at[h, z],
                    s9.at[h * 4 + n], r9.at[h * 4 + n], z_dev(n),
                )
            else:
                c = remote(
                    ps.at[h, lax.rem(y + n, 4)], ts.at[h, y],
                    s9.at[h * 4 + n], r9.at[h * 4 + n], y_dev(n),
                )
            c.start()
            cs.append(c)
        second.append(cs)

    f_all = ft[...].reshape(768, 1024)
    for p in range(parts):
        for c, d in zip(direct[p], passed[p][1:]):
            c.wait_recv()
            d.start()
        for c in passed[p]:
            c.wait_recv()
        d_all = jnp.concatenate([dl[h].reshape(1024, 128) for h in PARTS[p]], axis=1)
        g = jnp.dot(f_all, d_all, preferred_element_type=F32)
        for i, h in enumerate(PARTS[p]):
            half = g[:, i * 128 : (i + 1) * 128].reshape(4, 4, 48, 128)
            gs[h] = half.astype(BF16)
            res[h] = half
            cs = []
            for n in range(1, 4):
                if h % 2 == 0:
                    c = remote(
                        gs.at[h, lax.rem(y + n, 4)], rs.at[h, y],
                        s8.at[h * 4 + n], r8.at[h * 4 + n], y_dev(n),
                    )
                else:
                    c = remote(
                        gs.at[h, :, lax.rem(z + n, 4)], rs.at[h, z],
                        s8.at[h * 4 + n], r8.at[h * 4 + n], z_dev(n),
                    )
                c.start()
                cs.append(c)
            first.append(cs)
        if p == 0:
            for c in xs:
                c.wait()
            t = p1[0]
            for i in range(1, 8):
                t = t + p1[i]
            p2[y] = t
            sy = []
            for n in range(1, 4):
                c = remote(p2.at[y], p2.at[y], s5.at[n], r5.at[n], y_dev(n))
                c.start()
                sy.append(c)
        if p >= 2:
            for h in PARTS[p - 2]:
                fold(h)
        if p == 2:
            for c in sy:
                c.wait()
            p3[z] = (p2[0] + p2[1]) + (p2[2] + p2[3])
            zs = []
            for n in range(1, 4):
                c = remote(p3.at[z], p3.at[z], s6.at[n], r6.at[n], z_dev(n))
                c.start()
                zs.append(c)
        if p == 3:
            for c in zs:
                c.wait()
            small[j] = (p3[0] + p3[1]) + (p3[2] + p3[3])
            fin = []
            for n in range(1, 8):
                c = remote(
                    small.at[j], small.at[j], s7.at[n], r7.at[n], group_peer(seq, x, core, n)
                )
                c.start()
                fin.append(c)
    for h in PARTS[parts - 2] + PARTS[parts - 1]:
        fold(h)
    for p in range(parts):
        for c in direct[p] + passed[p]:
            c.wait_send()
    for h in range(8):
        for c in second[h]:
            c.wait()
        if h % 2 == 0:
            t = ps[h, z]
            for n in range(1, 4):
                t = t + ts[h, lax.rem(z + n, 4)]
        else:
            t = ps[h, y]
            for n in range(1, 4):
                t = t + ts[h, lax.rem(y + n, 4)]
        out[:, h * 128 : (h + 1) * 128] = t
    for c in fin:
        c.wait()


def reduce_all(norm, mass, pre, b_in, wo, bo, live, ft):
    dma = pltpu.SemaphoreType.DMA
    vmem = pl.BlockSpec(memory_space=VM)
    smem = pl.BlockSpec(memory_space=pltpu.SMEM)
    return pl.pallas_call(
        functools.partial(reduce_kernel, norm),
        name="reduce_all",
        out_shape=(
            jax.ShapeDtypeStruct((48, 1024), F32),
            jax.ShapeDtypeStruct((8, 8, 256), F32),
        ),
        in_specs=[vmem, vmem, vmem, vmem, smem, vmem, vmem],
        out_specs=(vmem,) * 2,
        scratch_shapes=[
            VM((4, 8, 128), F32), VM((8, 8, 128), F32), VM((8, 8, 128), F32),
            VM((8, 8, 128, 128), BF16),
            VM((8, 4, 4, 48, 128), BF16),
            VM((8, 4, 4, 48, 128), F32),
            VM((8, 4, 4, 48, 128), BF16),
            VM((8, 4, 48, 128), F32),
            VM((8, 4, 48, 128), F32),
            VM((8, 8, 256), F32), VM((8, 8, 256), F32), VM((4, 8, 256), F32), VM((4, 8, 256), F32),
        ]
        + [dma((4,)), dma((4,)), dma((8,)), dma((8,)), dma((40,)), dma((40,)), dma((8,)), dma((8,))]
        + [dma((4,)), dma((4,)), dma((4,)), dma((4,)), dma((8,)), dma((8,))]
        + [dma((32,)), dma((32,)), dma((32,)), dma((32,))],
        compiler_params=pltpu.CompilerParams(
            collective_id=1, has_side_effects=True, vmem_limit_bytes=40 * 2**20
        ),
    )(mass, pre, b_in, wo, bo, live, ft)


def finish_kernel(g, small, grad, bias, term, last):
    grad[...] = g[...]
    bias[...] = small[4, :, 128:256]
    t = jnp.concatenate([small[i] for i in range(4)], axis=1)
    term[...] = t
    r = jnp.concatenate([small[4, :, 0:128], jnp.zeros((120, 128), F32)], axis=0).T
    last[...] = jnp.sum(r, axis=0, keepdims=True)[:, 0:8]


def finish(g, small):
    vmem = pl.BlockSpec(memory_space=VM)
    return pl.pallas_call(
        finish_kernel,
        name="finish",
        out_shape=(
            jax.ShapeDtypeStruct((48, 1024), F32),
            jax.ShapeDtypeStruct((8, 128), F32),
            jax.ShapeDtypeStruct((8, 1024), F32),
            jax.ShapeDtypeStruct((1, 8), F32),
        ),
        in_specs=[vmem] * 2,
        out_specs=(vmem,) * 4,
        compiler_params=pltpu.CompilerParams(vmem_limit_bytes=8 * 2**20),
    )(g, small)


def on_device(queries, keys, values, lengths, block_pos, w_in, b_in, output_weight, output_bias):
    norm = 1.0 / math.sqrt(4 * 4096)
    qg, kg, ft, pre = spread(queries[0], keys[0], values[0], w_in)
    mass, live = column_mass(block_pos[0], lengths, qg, kg)
    g, small = reduce_all(
        norm, mass.reshape(4, 8, 128), pre, b_in[None, :], output_weight.T, output_bias, live, ft
    )
    grad, bias, term, last = finish(g, small)
    return (grad, bias.reshape(1024), term.T, last.reshape(8))


def solution(mesh):
    return jax.shard_map(
        on_device,
        mesh=mesh,
        in_specs=(
            P("batch", "seq", None),
            P("batch", "seq", None),
            P("batch", "seq", None),
            P("batch"),
            P("batch", None),
            P(),
            P(),
            P(),
            P(),
        ),
        out_specs=(P(("seq", "batch"), None), P(), P(), P()),
        check_vma=False,
    )
```

```python
import functools
import math

import jax
import jax.numpy as jnp
from jax import lax
from jax.experimental import pallas as pl
from jax.experimental.pallas import tpu as pltpu
from jax.sharding import PartitionSpec as P

MESH = pl.DeviceIdType.MESH
F32 = jnp.float32
BF16 = jnp.bfloat16
VM = pltpu.VMEM
CK = 512
WK = 512
KW = 2
PARTS = ((0, 1), (2, 3), (4, 5), (6, 7))
EARLY = 1
FP = 1


def place():
    seq = lax.axis_index("seq")
    x = lax.axis_index("batch")
    y = seq // 8
    row = lax.rem(seq, 8)
    core = lax.rem(seq, 2)
    return seq, x, y, row, core


def greet(seq, x, y, row, core):
    bar = pltpu.get_barrier_semaphore()
    n = 0
    near = [(y * 8 + lax.rem(row + k, 8), x) for k in range(1, 8)]
    near += [(lax.rem(y + k, 4) * 8 + row, x) for k in range(1, 4)]
    for dev in near:
        pl.semaphore_signal(bar, inc=1, device_id=dev, device_id_type=MESH)
        n += 1
    for k in range(1, 8):
        pl.semaphore_signal(bar, inc=1, device_id=group_peer(seq, x, core, k), device_id_type=MESH)
        n += 1
    return functools.partial(pl.semaphore_wait, bar, n)


def group_rank(x, core):
    return core * 4 + x


def group_peer(seq, x, core, k):
    j = lax.rem(group_rank(x, core) + k, 8)
    return (seq - core + j // 4, lax.rem(j, 4))


def remote(src, dst, ss, rs, dev):
    return pltpu.make_async_remote_copy(
        src_ref=src, dst_ref=dst, send_sem=ss, recv_sem=rs, device_id=dev, device_id_type=MESH
    )


def spread_kernel(
    q, k, v, w_hbm, qg, kg, ft_all, pre,
    ft, wbuf, wsem, ks, kr, qs, qr, fs, fr, ys, yr, ls,
):
    seq, x, y, row, core = place()
    j = group_rank(x, core)
    chunks = w_hbm.shape[0] // WK

    def fetch(i):
        return pltpu.make_async_copy(
            w_hbm.at[pl.ds(i * WK, WK)], wbuf.at[i % 3], wsem.at[i % 3]
        )

    fetch(0).start()
    fetch(1).start()
    met = greet(seq, x, y, row, core)
    lanes = pl.ds(pl.multiple_of(j * 128, 128), 128)
    kc, qc, fc, yc, own_f = [], [], [], [], []
    span = 16 // FP

    def turn(part):
        for i in range(part * span, part * span + span):
            pieces = []
            for t in range(3):
                col = i * 384 + t * 128
                if col < 4096:
                    pieces.append(q[:, col : col + 128])
                elif col < 5120:
                    pieces.append(k[:, col - 4096 : col - 3968])
                else:
                    pieces.append(v[:, col - 5120 : col - 4992])
            block = jnp.concatenate(pieces, axis=1).astype(F32).T.astype(BF16)
            for t in range(8):
                ft[i, t] = block[t * 48 : (t + 1) * 48]

    def send(part):
        some = pl.ds(part * span, span)
        for n in (2, 6, 1, 3, 5, 7, 4):
            to = lax.rem(j + n, 8)
            c = remote(
                ft.at[some, to], ft_all.at[some, :, lanes],
                fs.at[part * 8 + n], fr.at[part * 8 + n], group_peer(seq, x, core, n),
            )
            c.start()
            fc.append(c)
        c = pltpu.make_async_copy(ft.at[some, j], ft_all.at[some, :, lanes], ls.at[2 + part])
        c.start()
        own_f.append(c)

    for part in range(EARLY):
        turn(part)
    met()
    for n in range(4):
        cs = []
        for flip in range(2):
            if n == 0 and flip == 0:
                continue
            to = lax.rem(row // 2 + n, 4) * 2 + lax.rem(core + flip, 2)
            c = remote(
                k.at[:, pl.ds(pl.multiple_of(to * 128, 128), 128)], kg.at[seq],
                ks.at[n * 2 + flip], kr.at[n * 2 + flip], (y * 8 + to, x),
            )
            c.start()
            cs.append(c)
        kc.append(cs)
    own_k = pltpu.make_async_copy(
        k.at[:, pl.ds(pl.multiple_of(row * 128, 128), 128)], kg.at[seq], ls.at[0]
    )
    own_k.start()
    for part in range(EARLY):
        send(part)
    for n in range(1, 8):
        to = lax.rem(row + n, 8)
        c = remote(
            q.at[:, pl.ds(pl.multiple_of(to * 512, 512), 512)], qg.at[row],
            qs.at[n], qr.at[n], (y * 8 + to, x),
        )
        c.start()
        qc.append(c)
    own_q = pltpu.make_async_copy(
        q.at[:, pl.ds(pl.multiple_of(row * 512, 512), 512)], qg.at[row], ls.at[1]
    )
    own_q.start()
    for part in range(EARLY, FP):
        turn(part)
        send(part)

    def multiply(i):
        if i + 2 < chunks:
            fetch(i + 2).start()
        fetch(i).wait()
        lo = i * WK
        if lo < 4096:
            a = q[:, lo : lo + WK]
        elif lo < 5120:
            a = k[:, lo - 4096 : lo - 4096 + WK]
        else:
            a = v[:, lo - 5120 : lo - 5120 + WK]
        part = jnp.dot(a, wbuf[i % 3], preferred_element_type=F32)
        pre[...] = part if i == 0 else pre[...] + part

    def pass_on(n):
        pair = kg.at[pl.ds(y * 8 + lax.rem(row // 2 + 4 - n, 4) * 2, 2)]
        for m in (2, 1, 3):
            c = remote(
                pair, pair, ys.at[n * 4 + m], yr.at[n * 4 + m],
                (lax.rem(y + m, 4) * 8 + row, x),
            )
            c.start()
            yc.append(c)

    own_k.wait()
    for n in range(4):
        for c in kc[n]:
            c.wait_recv()
        pass_on(n)
        if n < KW:
            multiply(n)
    for i in range(KW, chunks):
        multiply(i)
    for c in qc + fc + yc:
        c.wait()
    for cs in kc:
        for c in cs:
            c.wait_send()
    own_q.wait()
    for c in own_f:
        c.wait()


def spread(q, k, v, w):
    dma = pltpu.SemaphoreType.DMA
    vmem = pl.BlockSpec(memory_space=VM)
    hbm = pl.BlockSpec(memory_space=pltpu.HBM)
    return pl.pallas_call(
        spread_kernel,
        name="spread",
        out_shape=(
            jax.ShapeDtypeStruct((8, 128, 512), BF16),
            jax.ShapeDtypeStruct((32, 128, 128), BF16),
            jax.ShapeDtypeStruct((16, 48, 1024), BF16),
            jax.ShapeDtypeStruct((128, 1024), F32),
        ),
        in_specs=[vmem, vmem, vmem, hbm],
        out_specs=(vmem,) * 4,
        scratch_shapes=[
            VM((16, 8, 48, 128), BF16),
            VM((3, WK, 1024), BF16),
            dma((3,)),
            dma((8,)), dma((8,)), dma((8,)), dma((8,)),
            dma((8 * FP,)), dma((8 * FP,)), dma((16,)), dma((16,)),
            dma((2 + FP,)),
        ],
        compiler_params=pltpu.CompilerParams(
            collective_id=0, has_side_effects=True, vmem_limit_bytes=40 * 2**20
        ),
    )(q, k, v, w)


def mass_kernel(meta, length, qg, kg, out, live, kpos, s_ref, acc):
    seq, _, y, _, _ = place()
    limit = length[0]
    first = y * 8
    here = lax.broadcasted_iota(jnp.int32, (1, 128), 1) + meta[seq] * 128
    live[...] = (here < limit).astype(F32)
    factor = math.log2(math.e) / math.sqrt(128)

    def order(r, _):
        for t in range(8):
            kpos[pl.ds(pl.multiple_of(meta[r * 8 + t] * 128, 128), 128)] = kg[r * 8 + t]
        return 0

    lax.fori_loop(0, 4, order, 0)
    acc[...] = jnp.zeros_like(acc)
    lane = lax.rem(lax.broadcasted_iota(jnp.int32, (1, 512), 1), 128)
    sub = lax.broadcasted_iota(jnp.int32, (CK, 512), 0)

    def fold(a, op):
        return op(a.reshape(CK // 8, 8, 512), axis=0)

    def block(i, _):
        pos = meta[first + i]

        @pl.when(pos * 128 < limit)
        def _():
            last = pos * 128 // CK
            q4 = jnp.concatenate([qg[i, :, h * 128 : (h + 1) * 128] for h in range(4)], axis=0)

            def scores(c):
                rows = pl.ds(pl.multiple_of(c * CK, CK), CK)
                return rows, lax.dot_general(
                    kpos[rows], q4, (((1,), (1,)), ((), ())), preferred_element_type=F32
                )

            def first_pass(c, top):
                rows, s = scores(c)
                s_ref[rows] = s
                return jnp.maximum(top, fold(s, jnp.max))

            top = lax.fori_loop(0, last, first_pass, jnp.full((8, 512), -1e30, F32))
            rows, s = scores(last)
            s = jnp.where(sub + last * CK <= lane + pos * 128, s, -1e30)
            s_ref[rows] = s
            top = jnp.max(jnp.maximum(top, fold(s, jnp.max)), axis=0, keepdims=True)

            def second_pass(c, total):
                rows = pl.ds(pl.multiple_of(c * CK, CK), CK)
                e = jnp.exp2((s_ref[rows] - top) * factor)
                s_ref[rows] = e
                return total + fold(e, jnp.sum)

            total = lax.fori_loop(0, last + 1, second_pass, jnp.zeros((8, 512), F32))
            total = jnp.sum(total, axis=0, keepdims=True)
            share = jnp.where(lane + pos * 128 < limit, 1.0 / total, 0.0)

            def third_pass(c, _):
                rows = pl.ds(pl.multiple_of(c * CK, CK), CK)
                e = s_ref[rows] * share
                acc[rows] += (e[:, 0:128] + e[:, 128:256]) + (e[:, 256:384] + e[:, 384:512])
                return 0

            lax.fori_loop(0, last + 1, third_pass, 0)

        return 0

    lax.fori_loop(0, 8, block, 0)

    def give(r, _):
        for t in range(16):
            rows = acc[pl.ds(pl.multiple_of(meta[r * 16 + t] * 128, 128), 128)]
            out[pl.ds(r * 16 + t, 1)] = jnp.sum(rows.T, axis=0, keepdims=True)
        return 0

    lax.fori_loop(0, 2, give, 0)


def column_mass(order, length, qg, kg):
    smem = pl.BlockSpec(memory_space=pltpu.SMEM)
    vmem = pl.BlockSpec(memory_space=VM)
    return pl.pallas_call(
        mass_kernel,
        name="column_mass",
        out_shape=(jax.ShapeDtypeStruct((32, 128), F32), jax.ShapeDtypeStruct((1, 128), F32)),
        in_specs=[smem, smem, vmem, vmem],
        out_specs=(vmem, vmem),
        scratch_shapes=[VM((4096, 128), BF16), VM((4096, 512), F32), VM((4096, 128), F32)],
        compiler_params=pltpu.CompilerParams(vmem_limit_bytes=40 * 2**20),
    )(order, length, qg, kg)


def reduce_kernel(
    norm, mass, pre, b_in, wo, bo, live, ft, out, small,
    m1, m2s, m2, dl, gs, res, rs, ps, ts, pk, p1, p2, p3,
    s1, r1, s2, r2, s3, r3, s4, r4, s5, r5, s6, r6, s7, r7, s8, r8, s9, r9,
):
    seq, x, y, row, core = place()
    z = row // 2
    j = group_rank(x, core)
    greet(seq, x, y, row, core)()

    def y_dev(n):
        return (lax.rem(y + n, 4) * 8 + row, x)

    def z_dev(n):
        return (y * 8 + lax.rem(z + n, 4) * 2 + core, x)

    cs = []
    for n in range(1, 4):
        c = remote(mass.at[lax.rem(y + n, 4)], m1.at[y], s1.at[n], r1.at[n], y_dev(n))
        c.start()
        cs.append(c)
    m1[y] = mass[y]
    lin = pre[...] + b_in[...]
    sig = jax.nn.sigmoid(lin)
    act = (lin * sig).astype(BF16)
    slope = sig * (1.0 + lin * (1.0 - sig))
    wide_o = jnp.concatenate([wo[...], jnp.zeros((120, 1024), BF16)], axis=0)
    for c in cs:
        c.wait()
    total = (m1[0] + m1[1]) + (m1[2] + m1[3])
    for i in range(8):
        m2s[i] = jnp.broadcast_to(total[i : i + 1], (8, 128))
    cs = []
    for n in range(1, 8):
        to = lax.rem(row + n, 8)
        c = remote(m2s.at[to], m2.at[row], s2.at[n], r2.at[n], (y * 8 + to, x))
        c.start()
        cs.append(c)
    m2[row] = m2s[row]
    p8 = lax.dot_general(wide_o, act, (((1,), (1,)), ((), ())), preferred_element_type=F32)
    pred = jnp.concatenate([p8[g : g + 1] + bo[g] for g in range(8)], axis=0)
    for c in cs:
        c.wait()
    mass_t = jnp.concatenate([m2[g, 0:1] for g in range(8)], axis=0)
    label = jnp.log1p(mass_t)
    resid = ((pred - label) * live[...] * norm).astype(BF16).astype(F32)
    wide = jnp.concatenate([resid, jnp.zeros((120, 128), F32)], axis=0)
    back = jnp.dot(wide.T.astype(BF16), wide_o, preferred_element_type=F32)
    delta = (back * slope).astype(BF16)
    other = (seq + 1 - 2 * core, x)
    base = core * 4
    for h in range(8):
        dl[h, j] = delta[:, h * 128 : (h + 1) * 128]
    parts = len(PARTS)

    def give(p, slot, n, dev):
        some = dl.at[pl.ds(PARTS[p][0], len(PARTS[p])), slot]
        return remote(some, some, s3.at[p * 8 + n], r3.at[p * 8 + n], dev)

    direct = [[give(p, j, n, (seq, lax.rem(x + n, 4))) for n in (2, 1, 3)] for p in range(parts)]
    passed = [
        [give(p, base + lax.rem(x + 4 - n, 4), 4 + n, other) for n in (0, 2, 1, 3)]
        for p in range(parts)
    ]

    def set_out(p):
        for c in direct[p]:
            c.start()
        passed[p][0].start()

    set_out(0)
    term = jnp.dot(wide.astype(BF16), act, preferred_element_type=F32)[0:8]
    bias = jnp.sum(delta.astype(F32), axis=0, keepdims=True)
    for i in range(4):
        pk[i] = term[:, i * 256 : (i + 1) * 256]
    pk[4, :, 0:128] = resid
    for i in range(8):
        pk[4, i : i + 1, 128:256] = bias[:, i * 128 : (i + 1) * 128]
    for i in range(5, 8):
        pk[i] = jnp.zeros((8, 256), F32)
    xs = []
    for n in range(1, 8):
        c = remote(
            pk.at[lax.rem(j + n, 8)], p1.at[j], s4.at[n], r4.at[n], group_peer(seq, x, core, n)
        )
        c.start()
        xs.append(c)
    p1[j] = pk[j]
    for p in range(1, parts):
        set_out(p)

    first, second = [], []

    def fold(h):
        for c in first[h]:
            c.wait()
        if h % 2 == 0:
            t = res[h, y]
            for n in range(1, 4):
                t = t + rs[h, lax.rem(y + n, 4)].astype(F32)
        else:
            t = res[h, :, z]
            for n in range(1, 4):
                t = t + rs[h, lax.rem(z + n, 4)].astype(F32)
        ps[h] = t
        cs = []
        for n in (2, 1, 3):
            if h % 2 == 0:
                c = remote(
                    ps.at[h, lax.rem(z + n, 4)], ts.at[h, z],
                    s9.at[h * 4 + n], r9.at[h * 4 + n], z_dev(n),
                )
            else:
                c = remote(
                    ps.at[h, lax.rem(y + n, 4)], ts.at[h, y],
                    s9.at[h * 4 + n], r9.at[h * 4 + n], y_dev(n),
                )
            c.start()
            cs.append(c)
        second.append(cs)

    f_all = ft[...].reshape(768, 1024)
    for p in range(parts):
        for c, d in zip(direct[p], passed[p][1:]):
            c.wait_recv()
            d.start()
        if p >= 2:
            for h in PARTS[p - 2]:
                fold(h)
        for c in passed[p]:
            c.wait_recv()
        d_all = jnp.concatenate([dl[h].reshape(1024, 128) for h in PARTS[p]], axis=1)
        g = jnp.dot(f_all, d_all, preferred_element_type=F32)
        for i, h in enumerate(PARTS[p]):
            half = g[:, i * 128 : (i + 1) * 128].reshape(4, 4, 48, 128)
            gs[h] = half.astype(BF16)
            res[h] = half
            cs = []
            for n in (2, 1, 3):
                if h % 2 == 0:
                    c = remote(
                        gs.at[h, lax.rem(y + n, 4)], rs.at[h, y],
                        s8.at[h * 4 + n], r8.at[h * 4 + n], y_dev(n),
                    )
                else:
                    c = remote(
                        gs.at[h, :, lax.rem(z + n, 4)], rs.at[h, z],
                        s8.at[h * 4 + n], r8.at[h * 4 + n], z_dev(n),
                    )
                c.start()
                cs.append(c)
            first.append(cs)
        if p == 0:
            for c in xs:
                c.wait()
            t = p1[0]
            for i in range(1, 8):
                t = t + p1[i]
            p2[y] = t
            sy = []
            for n in range(1, 4):
                c = remote(p2.at[y], p2.at[y], s5.at[n], r5.at[n], y_dev(n))
                c.start()
                sy.append(c)
        if p == 2:
            for c in sy:
                c.wait()
            p3[z] = (p2[0] + p2[1]) + (p2[2] + p2[3])
            zs = []
            for n in range(1, 4):
                c = remote(p3.at[z], p3.at[z], s6.at[n], r6.at[n], z_dev(n))
                c.start()
                zs.append(c)
        if p == 3:
            for c in zs:
                c.wait()
            small[j] = (p3[0] + p3[1]) + (p3[2] + p3[3])
            fin = []
            for n in range(1, 8):
                c = remote(
                    small.at[j], small.at[j], s7.at[n], r7.at[n], group_peer(seq, x, core, n)
                )
                c.start()
                fin.append(c)
    for h in PARTS[parts - 2] + PARTS[parts - 1]:
        fold(h)
    for p in range(parts):
        for c in direct[p] + passed[p]:
            c.wait_send()
    for h in range(8):
        for c in second[h]:
            c.wait()
        if h % 2 == 0:
            t = ps[h, z]
            for n in range(1, 4):
                t = t + ts[h, lax.rem(z + n, 4)]
        else:
            t = ps[h, y]
            for n in range(1, 4):
                t = t + ts[h, lax.rem(y + n, 4)]
        out[:, h * 128 : (h + 1) * 128] = t
    for c in fin:
        c.wait()


def reduce_all(norm, mass, pre, b_in, wo, bo, live, ft):
    dma = pltpu.SemaphoreType.DMA
    vmem = pl.BlockSpec(memory_space=VM)
    smem = pl.BlockSpec(memory_space=pltpu.SMEM)
    return pl.pallas_call(
        functools.partial(reduce_kernel, norm),
        name="reduce_all",
        out_shape=(
            jax.ShapeDtypeStruct((48, 1024), F32),
            jax.ShapeDtypeStruct((8, 8, 256), F32),
        ),
        in_specs=[vmem, vmem, vmem, vmem, smem, vmem, vmem],
        out_specs=(vmem,) * 2,
        scratch_shapes=[
            VM((4, 8, 128), F32), VM((8, 8, 128), F32), VM((8, 8, 128), F32),
            VM((8, 8, 128, 128), BF16),
            VM((8, 4, 4, 48, 128), BF16),
            VM((8, 4, 4, 48, 128), F32),
            VM((8, 4, 4, 48, 128), BF16),
            VM((8, 4, 48, 128), F32),
            VM((8, 4, 48, 128), F32),
            VM((8, 8, 256), F32), VM((8, 8, 256), F32), VM((4, 8, 256), F32), VM((4, 8, 256), F32),
        ]
        + [dma((4,)), dma((4,)), dma((8,)), dma((8,)), dma((40,)), dma((40,)), dma((8,)), dma((8,))]
        + [dma((4,)), dma((4,)), dma((4,)), dma((4,)), dma((8,)), dma((8,))]
        + [dma((32,)), dma((32,)), dma((32,)), dma((32,))],
        compiler_params=pltpu.CompilerParams(
            collective_id=1, has_side_effects=True, vmem_limit_bytes=40 * 2**20
        ),
    )(mass, pre, b_in, wo, bo, live, ft)


def finish_kernel(g, small, grad, bias, term, last):
    grad[...] = g[...]
    bias[...] = small[4, :, 128:256]
    t = jnp.concatenate([small[i] for i in range(4)], axis=1)
    term[...] = t
    r = jnp.concatenate([small[4, :, 0:128], jnp.zeros((120, 128), F32)], axis=0).T
    last[...] = jnp.sum(r, axis=0, keepdims=True)[:, 0:8]


def finish(g, small):
    vmem = pl.BlockSpec(memory_space=VM)
    return pl.pallas_call(
        finish_kernel,
        name="finish",
        out_shape=(
            jax.ShapeDtypeStruct((48, 1024), F32),
            jax.ShapeDtypeStruct((8, 128), F32),
            jax.ShapeDtypeStruct((8, 1024), F32),
            jax.ShapeDtypeStruct((1, 8), F32),
        ),
        in_specs=[vmem] * 2,
        out_specs=(vmem,) * 4,
        compiler_params=pltpu.CompilerParams(vmem_limit_bytes=8 * 2**20),
    )(g, small)


def on_device(queries, keys, values, lengths, block_pos, w_in, b_in, output_weight, output_bias):
    norm = 1.0 / math.sqrt(4 * 4096)
    qg, kg, ft, pre = spread(queries[0], keys[0], values[0], w_in)
    mass, live = column_mass(block_pos[0], lengths, qg, kg)
    g, small = reduce_all(
        norm, mass.reshape(4, 8, 128), pre, b_in[None, :], output_weight.T, output_bias, live, ft
    )
    grad, bias, term, last = finish(g, small)
    return (grad, bias.reshape(1024), term.T, last.reshape(8))


def solution(mesh):
    return jax.shard_map(
        on_device,
        mesh=mesh,
        in_specs=(
            P("batch", "seq", None),
            P("batch", "seq", None),
            P("batch", "seq", None),
            P("batch"),
            P("batch", None),
            P(),
            P(),
            P(),
            P(),
        ),
        out_specs=(P(("seq", "batch"), None), P(), P(), P()),
        check_vma=False,
    )
```

```python
import functools
import math

import jax
import jax.numpy as jnp
from jax import lax
from jax.experimental import pallas as pl
from jax.experimental.pallas import tpu as pltpu
from jax.sharding import PartitionSpec as P

MESH = pl.DeviceIdType.MESH
F32 = jnp.float32
BF16 = jnp.bfloat16
VM = pltpu.VMEM
CK = 1024
WK = 512
KW = 2
PARTS = ((0, 1), (2, 3), (4, 5), (6, 7))
EARLY = 1
FP = 1


def place():
    seq = lax.axis_index("seq")
    x = lax.axis_index("batch")
    y = seq // 8
    row = lax.rem(seq, 8)
    core = lax.rem(seq, 2)
    return seq, x, y, row, core


def greet(seq, x, y, row, core):
    bar = pltpu.get_barrier_semaphore()
    n = 0
    near = [(y * 8 + lax.rem(row + k, 8), x) for k in range(1, 8)]
    near += [(lax.rem(y + k, 4) * 8 + row, x) for k in range(1, 4)]
    for dev in near:
        pl.semaphore_signal(bar, inc=1, device_id=dev, device_id_type=MESH)
        n += 1
    for k in range(1, 8):
        pl.semaphore_signal(bar, inc=1, device_id=group_peer(seq, x, core, k), device_id_type=MESH)
        n += 1
    return functools.partial(pl.semaphore_wait, bar, n)


def group_rank(x, core):
    return core * 4 + x


def group_peer(seq, x, core, k):
    j = lax.rem(group_rank(x, core) + k, 8)
    return (seq - core + j // 4, lax.rem(j, 4))


def remote(src, dst, ss, rs, dev):
    return pltpu.make_async_remote_copy(
        src_ref=src, dst_ref=dst, send_sem=ss, recv_sem=rs, device_id=dev, device_id_type=MESH
    )


def spread_kernel(
    q, k, v, w_hbm, qg, kg, ft_all, pre,
    ft, wbuf, wsem, ks, kr, qs, qr, fs, fr, ys, yr, ls,
):
    seq, x, y, row, core = place()
    j = group_rank(x, core)
    chunks = w_hbm.shape[0] // WK

    def fetch(i):
        return pltpu.make_async_copy(
            w_hbm.at[pl.ds(i * WK, WK)], wbuf.at[i % 3], wsem.at[i % 3]
        )

    fetch(0).start()
    fetch(1).start()
    met = greet(seq, x, y, row, core)
    lanes = pl.ds(pl.multiple_of(j * 128, 128), 128)
    kc, qc, fc, yc, own_f = [], [], [], [], []
    span = 16 // FP

    def turn(part):
        for i in range(part * span, part * span + span):
            pieces = []
            for t in range(3):
                col = i * 384 + t * 128
                if col < 4096:
                    pieces.append(q[:, col : col + 128])
                elif col < 5120:
                    pieces.append(k[:, col - 4096 : col - 3968])
                else:
                    pieces.append(v[:, col - 5120 : col - 4992])
            block = jnp.concatenate(pieces, axis=1).astype(F32).T.astype(BF16)
            for t in range(8):
                ft[i, t] = block[t * 48 : (t + 1) * 48]

    def send(part):
        some = pl.ds(part * span, span)
        for n in (2, 6, 1, 3, 5, 7, 4):
            to = lax.rem(j + n, 8)
            c = remote(
                ft.at[some, to], ft_all.at[some, :, lanes],
                fs.at[part * 8 + n], fr.at[part * 8 + n], group_peer(seq, x, core, n),
            )
            c.start()
            fc.append(c)
        c = pltpu.make_async_copy(ft.at[some, j], ft_all.at[some, :, lanes], ls.at[2 + part])
        c.start()
        own_f.append(c)

    for part in range(EARLY):
        turn(part)
    met()
    for n in range(4):
        cs = []
        for flip in range(2):
            if n == 0 and flip == 0:
                continue
            to = lax.rem(row // 2 + n, 4) * 2 + lax.rem(core + flip, 2)
            c = remote(
                k.at[:, pl.ds(pl.multiple_of(to * 128, 128), 128)], kg.at[seq],
                ks.at[n * 2 + flip], kr.at[n * 2 + flip], (y * 8 + to, x),
            )
            c.start()
            cs.append(c)
        kc.append(cs)
    own_k = pltpu.make_async_copy(
        k.at[:, pl.ds(pl.multiple_of(row * 128, 128), 128)], kg.at[seq], ls.at[0]
    )
    own_k.start()
    for part in range(EARLY):
        send(part)
    for n in range(1, 8):
        to = lax.rem(row + n, 8)
        c = remote(
            q.at[:, pl.ds(pl.multiple_of(to * 512, 512), 512)], qg.at[row],
            qs.at[n], qr.at[n], (y * 8 + to, x),
        )
        c.start()
        qc.append(c)
    own_q = pltpu.make_async_copy(
        q.at[:, pl.ds(pl.multiple_of(row * 512, 512), 512)], qg.at[row], ls.at[1]
    )
    own_q.start()
    for part in range(EARLY, FP):
        turn(part)
        send(part)

    def multiply(i):
        if i + 2 < chunks:
            fetch(i + 2).start()
        fetch(i).wait()
        lo = i * WK
        if lo < 4096:
            a = q[:, lo : lo + WK]
        elif lo < 5120:
            a = k[:, lo - 4096 : lo - 4096 + WK]
        else:
            a = v[:, lo - 5120 : lo - 5120 + WK]
        part = jnp.dot(a, wbuf[i % 3], preferred_element_type=F32)
        pre[...] = part if i == 0 else pre[...] + part

    def pass_on(n):
        pair = kg.at[pl.ds(y * 8 + lax.rem(row // 2 + 4 - n, 4) * 2, 2)]
        for m in (2, 1, 3):
            c = remote(
                pair, pair, ys.at[n * 4 + m], yr.at[n * 4 + m],
                (lax.rem(y + m, 4) * 8 + row, x),
            )
            c.start()
            yc.append(c)

    own_k.wait()
    for n in range(4):
        for c in kc[n]:
            c.wait_recv()
        pass_on(n)
        if n < KW:
            multiply(n)
    for i in range(KW, chunks):
        multiply(i)
    for c in qc + fc + yc:
        c.wait()
    for cs in kc:
        for c in cs:
            c.wait_send()
    own_q.wait()
    for c in own_f:
        c.wait()


def spread(q, k, v, w):
    dma = pltpu.SemaphoreType.DMA
    vmem = pl.BlockSpec(memory_space=VM)
    hbm = pl.BlockSpec(memory_space=pltpu.HBM)
    return pl.pallas_call(
        spread_kernel,
        name="spread",
        out_shape=(
            jax.ShapeDtypeStruct((8, 128, 512), BF16),
            jax.ShapeDtypeStruct((32, 128, 128), BF16),
            jax.ShapeDtypeStruct((16, 48, 1024), BF16),
            jax.ShapeDtypeStruct((128, 1024), F32),
        ),
        in_specs=[vmem, vmem, vmem, hbm],
        out_specs=(vmem,) * 4,
        scratch_shapes=[
            VM((16, 8, 48, 128), BF16),
            VM((3, WK, 1024), BF16),
            dma((3,)),
            dma((8,)), dma((8,)), dma((8,)), dma((8,)),
            dma((8 * FP,)), dma((8 * FP,)), dma((16,)), dma((16,)),
            dma((2 + FP,)),
        ],
        compiler_params=pltpu.CompilerParams(
            collective_id=0, has_side_effects=True, vmem_limit_bytes=40 * 2**20
        ),
    )(q, k, v, w)


def mass_kernel(meta, length, qg, kg, out, live, kpos, s_ref, acc):
    seq, _, y, _, _ = place()
    limit = length[0]
    first = y * 8
    here = lax.broadcasted_iota(jnp.int32, (1, 128), 1) + meta[seq] * 128
    live[...] = (here < limit).astype(F32)
    factor = math.log2(math.e) / math.sqrt(128)

    def order(r, _):
        for t in range(8):
            kpos[pl.ds(pl.multiple_of(meta[r * 8 + t] * 128, 128), 128)] = kg[r * 8 + t]
        return 0

    lax.fori_loop(0, 4, order, 0)
    acc[...] = jnp.zeros_like(acc)
    lane = lax.rem(lax.broadcasted_iota(jnp.int32, (1, 512), 1), 128)
    sub = lax.broadcasted_iota(jnp.int32, (CK, 512), 0)

    def fold(a, op):
        return op(a.reshape(CK // 8, 8, 512), axis=0)

    def block(i, _):
        pos = meta[first + i]

        @pl.when(pos * 128 < limit)
        def _():
            last = pos * 128 // CK
            q4 = jnp.concatenate([qg[i, :, h * 128 : (h + 1) * 128] for h in range(4)], axis=0)

            def scores(c):
                rows = pl.ds(pl.multiple_of(c * CK, CK), CK)
                return rows, lax.dot_general(
                    kpos[rows], q4, (((1,), (1,)), ((), ())), preferred_element_type=F32
                )

            def first_pass(c, top):
                rows, s = scores(c)
                s_ref[rows] = s
                return jnp.maximum(top, fold(s, jnp.max))

            top = lax.fori_loop(0, last, first_pass, jnp.full((8, 512), -1e30, F32))
            rows, s = scores(last)
            s = jnp.where(sub + last * CK <= lane + pos * 128, s, -1e30)
            s_ref[rows] = s
            top = jnp.max(jnp.maximum(top, fold(s, jnp.max)), axis=0, keepdims=True)

            def second_pass(c, total):
                rows = pl.ds(pl.multiple_of(c * CK, CK), CK)
                e = jnp.exp2((s_ref[rows] - top) * factor)
                s_ref[rows] = e
                return total + fold(e, jnp.sum)

            total = lax.fori_loop(0, last + 1, second_pass, jnp.zeros((8, 512), F32))
            total = jnp.sum(total, axis=0, keepdims=True)
            share = jnp.where(lane + pos * 128 < limit, 1.0 / total, 0.0)

            def third_pass(c, _):
                rows = pl.ds(pl.multiple_of(c * CK, CK), CK)
                e = s_ref[rows] * share
                acc[rows] += (e[:, 0:128] + e[:, 128:256]) + (e[:, 256:384] + e[:, 384:512])
                return 0

            lax.fori_loop(0, last + 1, third_pass, 0)

        return 0

    lax.fori_loop(0, 8, block, 0)

    def give(r, _):
        for t in range(16):
            rows = acc[pl.ds(pl.multiple_of(meta[r * 16 + t] * 128, 128), 128)]
            out[pl.ds(r * 16 + t, 1)] = jnp.sum(rows.T, axis=0, keepdims=True)
        return 0

    lax.fori_loop(0, 2, give, 0)


def column_mass(order, length, qg, kg):
    smem = pl.BlockSpec(memory_space=pltpu.SMEM)
    vmem = pl.BlockSpec(memory_space=VM)
    return pl.pallas_call(
        mass_kernel,
        name="column_mass",
        out_shape=(jax.ShapeDtypeStruct((32, 128), F32), jax.ShapeDtypeStruct((1, 128), F32)),
        in_specs=[smem, smem, vmem, vmem],
        out_specs=(vmem, vmem),
        scratch_shapes=[VM((4096, 128), BF16), VM((4096, 512), F32), VM((4096, 128), F32)],
        compiler_params=pltpu.CompilerParams(vmem_limit_bytes=40 * 2**20),
    )(order, length, qg, kg)


def reduce_kernel(
    norm, mass, pre, b_in, wo, bo, live, ft, out, small,
    m1, m2s, m2, dl, gs, res, rs, ps, ts, pk, p1, p2, p3,
    s1, r1, s2, r2, s3, r3, s4, r4, s5, r5, s6, r6, s7, r7, s8, r8, s9, r9,
):
    seq, x, y, row, core = place()
    z = row // 2
    j = group_rank(x, core)
    greet(seq, x, y, row, core)()

    def y_dev(n):
        return (lax.rem(y + n, 4) * 8 + row, x)

    def z_dev(n):
        return (y * 8 + lax.rem(z + n, 4) * 2 + core, x)

    cs = []
    for n in range(1, 4):
        c = remote(mass.at[lax.rem(y + n, 4)], m1.at[y], s1.at[n], r1.at[n], y_dev(n))
        c.start()
        cs.append(c)
    m1[y] = mass[y]
    lin = pre[...] + b_in[...]
    sig = jax.nn.sigmoid(lin)
    act = (lin * sig).astype(BF16)
    slope = sig * (1.0 + lin * (1.0 - sig))
    wide_o = jnp.concatenate([wo[...], jnp.zeros((120, 1024), BF16)], axis=0)
    for c in cs:
        c.wait()
    total = (m1[0] + m1[1]) + (m1[2] + m1[3])
    for i in range(8):
        m2s[i] = jnp.broadcast_to(total[i : i + 1], (8, 128))
    cs = []
    for n in range(1, 8):
        to = lax.rem(row + n, 8)
        c = remote(m2s.at[to], m2.at[row], s2.at[n], r2.at[n], (y * 8 + to, x))
        c.start()
        cs.append(c)
    m2[row] = m2s[row]
    p8 = lax.dot_general(wide_o, act, (((1,), (1,)), ((), ())), preferred_element_type=F32)
    pred = jnp.concatenate([p8[g : g + 1] + bo[g] for g in range(8)], axis=0)
    for c in cs:
        c.wait()
    mass_t = jnp.concatenate([m2[g, 0:1] for g in range(8)], axis=0)
    label = jnp.log1p(mass_t)
    resid = ((pred - label) * live[...] * norm).astype(BF16).astype(F32)
    wide = jnp.concatenate([resid, jnp.zeros((120, 128), F32)], axis=0)
    back = jnp.dot(wide.T.astype(BF16), wide_o, preferred_element_type=F32)
    delta = (back * slope).astype(BF16)
    other = (seq + 1 - 2 * core, x)
    base = core * 4
    for h in range(8):
        dl[h, j] = delta[:, h * 128 : (h + 1) * 128]
    parts = len(PARTS)

    def give(p, slot, n, dev):
        some = dl.at[pl.ds(PARTS[p][0], len(PARTS[p])), slot]
        return remote(some, some, s3.at[p * 8 + n], r3.at[p * 8 + n], dev)

    direct = [[give(p, j, n, (seq, lax.rem(x + n, 4))) for n in (2, 1, 3)] for p in range(parts)]
    passed = [
        [give(p, base + lax.rem(x + 4 - n, 4), 4 + n, other) for n in (0, 2, 1, 3)]
        for p in range(parts)
    ]

    def set_out(p):
        for c in direct[p]:
            c.start()
        passed[p][0].start()

    set_out(0)
    term = jnp.dot(wide.astype(BF16), act, preferred_element_type=F32)[0:8]
    bias = jnp.sum(delta.astype(F32), axis=0, keepdims=True)
    for i in range(4):
        pk[i] = term[:, i * 256 : (i + 1) * 256]
    pk[4, :, 0:128] = resid
    for i in range(8):
        pk[4, i : i + 1, 128:256] = bias[:, i * 128 : (i + 1) * 128]
    for i in range(5, 8):
        pk[i] = jnp.zeros((8, 256), F32)
    xs = []
    for n in range(1, 8):
        c = remote(
            pk.at[lax.rem(j + n, 8)], p1.at[j], s4.at[n], r4.at[n], group_peer(seq, x, core, n)
        )
        c.start()
        xs.append(c)
    p1[j] = pk[j]
    for p in range(1, parts):
        set_out(p)

    first, second = [], []

    def fold(h):
        for c in first[h]:
            c.wait()
        if h % 2 == 0:
            t = res[h, y]
            for n in range(1, 4):
                t = t + rs[h, lax.rem(y + n, 4)].astype(F32)
        else:
            t = res[h, :, z]
            for n in range(1, 4):
                t = t + rs[h, lax.rem(z + n, 4)].astype(F32)
        ps[h] = t
        cs = []
        for n in (2, 1, 3):
            if h % 2 == 0:
                c = remote(
                    ps.at[h, lax.rem(z + n, 4)], ts.at[h, z],
                    s9.at[h * 4 + n], r9.at[h * 4 + n], z_dev(n),
                )
            else:
                c = remote(
                    ps.at[h, lax.rem(y + n, 4)], ts.at[h, y],
                    s9.at[h * 4 + n], r9.at[h * 4 + n], y_dev(n),
                )
            c.start()
            cs.append(c)
        second.append(cs)

    f_all = ft[...].reshape(768, 1024)
    for p in range(parts):
        for c, d in zip(direct[p], passed[p][1:]):
            c.wait_recv()
            d.start()
        if p >= 2:
            for h in PARTS[p - 2]:
                fold(h)
        for c in passed[p]:
            c.wait_recv()
        d_all = jnp.concatenate([dl[h].reshape(1024, 128) for h in PARTS[p]], axis=1)
        g = jnp.dot(f_all, d_all, preferred_element_type=F32)
        for i, h in enumerate(PARTS[p]):
            half = g[:, i * 128 : (i + 1) * 128].reshape(4, 4, 48, 128)
            gs[h] = half.astype(BF16)
            res[h] = half
            cs = []
            for n in (2, 1, 3):
                if h % 2 == 0:
                    c = remote(
                        gs.at[h, lax.rem(y + n, 4)], rs.at[h, y],
                        s8.at[h * 4 + n], r8.at[h * 4 + n], y_dev(n),
                    )
                else:
                    c = remote(
                        gs.at[h, :, lax.rem(z + n, 4)], rs.at[h, z],
                        s8.at[h * 4 + n], r8.at[h * 4 + n], z_dev(n),
                    )
                c.start()
                cs.append(c)
            first.append(cs)
        if p == 0:
            for c in xs:
                c.wait()
            t = p1[0]
            for i in range(1, 8):
                t = t + p1[i]
            p2[y] = t
            sy = []
            for n in range(1, 4):
                c = remote(p2.at[y], p2.at[y], s5.at[n], r5.at[n], y_dev(n))
                c.start()
                sy.append(c)
        if p == 2:
            for c in sy:
                c.wait()
            p3[z] = (p2[0] + p2[1]) + (p2[2] + p2[3])
            zs = []
            for n in range(1, 4):
                c = remote(p3.at[z], p3.at[z], s6.at[n], r6.at[n], z_dev(n))
                c.start()
                zs.append(c)
        if p == 3:
            for c in zs:
                c.wait()
            small[j] = (p3[0] + p3[1]) + (p3[2] + p3[3])
            fin = []
            for n in range(1, 8):
                c = remote(
                    small.at[j], small.at[j], s7.at[n], r7.at[n], group_peer(seq, x, core, n)
                )
                c.start()
                fin.append(c)
    for h in PARTS[parts - 2] + PARTS[parts - 1]:
        fold(h)
    for p in range(parts):
        for c in direct[p] + passed[p]:
            c.wait_send()
    for h in range(8):
        for c in second[h]:
            c.wait()
        if h % 2 == 0:
            t = ps[h, z]
            for n in range(1, 4):
                t = t + ts[h, lax.rem(z + n, 4)]
        else:
            t = ps[h, y]
            for n in range(1, 4):
                t = t + ts[h, lax.rem(y + n, 4)]
        out[:, h * 128 : (h + 1) * 128] = t
    for c in fin:
        c.wait()


def reduce_all(norm, mass, pre, b_in, wo, bo, live, ft):
    dma = pltpu.SemaphoreType.DMA
    vmem = pl.BlockSpec(memory_space=VM)
    smem = pl.BlockSpec(memory_space=pltpu.SMEM)
    return pl.pallas_call(
        functools.partial(reduce_kernel, norm),
        name="reduce_all",
        out_shape=(
            jax.ShapeDtypeStruct((48, 1024), F32),
            jax.ShapeDtypeStruct((8, 8, 256), F32),
        ),
        in_specs=[vmem, vmem, vmem, vmem, smem, vmem, vmem],
        out_specs=(vmem,) * 2,
        scratch_shapes=[
            VM((4, 8, 128), F32), VM((8, 8, 128), F32), VM((8, 8, 128), F32),
            VM((8, 8, 128, 128), BF16),
            VM((8, 4, 4, 48, 128), BF16),
            VM((8, 4, 4, 48, 128), F32),
            VM((8, 4, 4, 48, 128), BF16),
            VM((8, 4, 48, 128), F32),
            VM((8, 4, 48, 128), F32),
            VM((8, 8, 256), F32), VM((8, 8, 256), F32), VM((4, 8, 256), F32), VM((4, 8, 256), F32),
        ]
        + [dma((4,)), dma((4,)), dma((8,)), dma((8,)), dma((40,)), dma((40,)), dma((8,)), dma((8,))]
        + [dma((4,)), dma((4,)), dma((4,)), dma((4,)), dma((8,)), dma((8,))]
        + [dma((32,)), dma((32,)), dma((32,)), dma((32,))],
        compiler_params=pltpu.CompilerParams(
            collective_id=1, has_side_effects=True, vmem_limit_bytes=40 * 2**20
        ),
    )(mass, pre, b_in, wo, bo, live, ft)


def finish_kernel(g, small, grad, bias, term, last):
    grad[...] = g[...]
    bias[...] = small[4, :, 128:256]
    t = jnp.concatenate([small[i] for i in range(4)], axis=1)
    term[...] = t
    r = jnp.concatenate([small[4, :, 0:128], jnp.zeros((120, 128), F32)], axis=0).T
    last[...] = jnp.sum(r, axis=0, keepdims=True)[:, 0:8]


def finish(g, small):
    vmem = pl.BlockSpec(memory_space=VM)
    return pl.pallas_call(
        finish_kernel,
        name="finish",
        out_shape=(
            jax.ShapeDtypeStruct((48, 1024), F32),
            jax.ShapeDtypeStruct((8, 128), F32),
            jax.ShapeDtypeStruct((8, 1024), F32),
            jax.ShapeDtypeStruct((1, 8), F32),
        ),
        in_specs=[vmem] * 2,
        out_specs=(vmem,) * 4,
        compiler_params=pltpu.CompilerParams(vmem_limit_bytes=8 * 2**20),
    )(g, small)


def on_device(queries, keys, values, lengths, block_pos, w_in, b_in, output_weight, output_bias):
    norm = 1.0 / math.sqrt(4 * 4096)
    qg, kg, ft, pre = spread(queries[0], keys[0], values[0], w_in)
    mass, live = column_mass(block_pos[0], lengths, qg, kg)
    g, small = reduce_all(
        norm, mass.reshape(4, 8, 128), pre, b_in[None, :], output_weight.T, output_bias, live, ft
    )
    grad, bias, term, last = finish(g, small)
    return (grad, bias.reshape(1024), term.T, last.reshape(8))


def solution(mesh):
    return jax.shard_map(
        on_device,
        mesh=mesh,
        in_specs=(
            P("batch", "seq", None),
            P("batch", "seq", None),
            P("batch", "seq", None),
            P("batch"),
            P("batch", None),
            P(),
            P(),
            P(),
            P(),
        ),
        out_specs=(P(("seq", "batch"), None), P(), P(), P()),
        check_vma=False,
    )
```

```python
import functools
import math

import jax
import jax.numpy as jnp
from jax import lax
from jax.experimental import pallas as pl
from jax.experimental.pallas import tpu as pltpu
from jax.sharding import PartitionSpec as P

MESH = pl.DeviceIdType.MESH
F32 = jnp.float32
BF16 = jnp.bfloat16
VM = pltpu.VMEM
CK = 1024
WK = 512
KW = 2
PARTS = ((0, 1), (2, 3), (4, 5), (6, 7))
EARLY = 1
FP = 1


def place():
    seq = lax.axis_index("seq")
    x = lax.axis_index("batch")
    y = seq // 8
    row = lax.rem(seq, 8)
    core = lax.rem(seq, 2)
    return seq, x, y, row, core


def greet(seq, x, y, row, core):
    bar = pltpu.get_barrier_semaphore()
    n = 0
    near = [(y * 8 + lax.rem(row + k, 8), x) for k in range(1, 8)]
    near += [(lax.rem(y + k, 4) * 8 + row, x) for k in range(1, 4)]
    for dev in near:
        pl.semaphore_signal(bar, inc=1, device_id=dev, device_id_type=MESH)
        n += 1
    for k in range(1, 8):
        pl.semaphore_signal(bar, inc=1, device_id=group_peer(seq, x, core, k), device_id_type=MESH)
        n += 1
    return functools.partial(pl.semaphore_wait, bar, n)


def group_rank(x, core):
    return core * 4 + x


def group_peer(seq, x, core, k):
    j = lax.rem(group_rank(x, core) + k, 8)
    return (seq - core + j // 4, lax.rem(j, 4))


def remote(src, dst, ss, rs, dev):
    return pltpu.make_async_remote_copy(
        src_ref=src, dst_ref=dst, send_sem=ss, recv_sem=rs, device_id=dev, device_id_type=MESH
    )


def spread_kernel(
    q, k, v, w_hbm, qg, kg, ft_all, pre,
    ft, wbuf, wsem, ks, kr, qs, qr, fs, fr, ys, yr, ls,
):
    seq, x, y, row, core = place()
    j = group_rank(x, core)
    chunks = w_hbm.shape[0] // WK

    def fetch(i):
        return pltpu.make_async_copy(
            w_hbm.at[pl.ds(i * WK, WK)], wbuf.at[i % 3], wsem.at[i % 3]
        )

    fetch(0).start()
    fetch(1).start()
    met = greet(seq, x, y, row, core)
    lanes = pl.ds(pl.multiple_of(j * 128, 128), 128)
    kc, qc, fc, yc, own_f = [], [], [], [], []
    span = 16 // FP

    def turn(part):
        for i in range(part * span, part * span + span):
            pieces = []
            for t in range(3):
                col = i * 384 + t * 128
                if col < 4096:
                    pieces.append(q[:, col : col + 128])
                elif col < 5120:
                    pieces.append(k[:, col - 4096 : col - 3968])
                else:
                    pieces.append(v[:, col - 5120 : col - 4992])
            block = jnp.concatenate(pieces, axis=1).astype(F32).T.astype(BF16)
            for t in range(8):
                ft[i, t] = block[t * 48 : (t + 1) * 48]

    def send(part):
        some = pl.ds(part * span, span)
        for n in (2, 6, 1, 3, 5, 7, 4):
            to = lax.rem(j + n, 8)
            c = remote(
                ft.at[some, to], ft_all.at[some, :, lanes],
                fs.at[part * 8 + n], fr.at[part * 8 + n], group_peer(seq, x, core, n),
            )
            c.start()
            fc.append(c)
        c = pltpu.make_async_copy(ft.at[some, j], ft_all.at[some, :, lanes], ls.at[2 + part])
        c.start()
        own_f.append(c)

    for part in range(EARLY):
        turn(part)
    met()
    for n in range(4):
        cs = []
        for flip in range(2):
            if n == 0 and flip == 0:
                continue
            to = lax.rem(row // 2 + n, 4) * 2 + lax.rem(core + flip, 2)
            c = remote(
                k.at[:, pl.ds(pl.multiple_of(to * 128, 128), 128)], kg.at[seq],
                ks.at[n * 2 + flip], kr.at[n * 2 + flip], (y * 8 + to, x),
            )
            c.start()
            cs.append(c)
        kc.append(cs)
    own_k = pltpu.make_async_copy(
        k.at[:, pl.ds(pl.multiple_of(row * 128, 128), 128)], kg.at[seq], ls.at[0]
    )
    own_k.start()
    for part in range(EARLY):
        send(part)
    for n in range(1, 8):
        to = lax.rem(row + n, 8)
        c = remote(
            q.at[:, pl.ds(pl.multiple_of(to * 512, 512), 512)], qg.at[row],
            qs.at[n], qr.at[n], (y * 8 + to, x),
        )
        c.start()
        qc.append(c)
    own_q = pltpu.make_async_copy(
        q.at[:, pl.ds(pl.multiple_of(row * 512, 512), 512)], qg.at[row], ls.at[1]
    )
    own_q.start()
    for part in range(EARLY, FP):
        turn(part)
        send(part)

    def multiply(i):
        if i + 2 < chunks:
            fetch(i + 2).start()
        fetch(i).wait()
        lo = i * WK
        if lo < 4096:
            a = q[:, lo : lo + WK]
        elif lo < 5120:
            a = k[:, lo - 4096 : lo - 4096 + WK]
        else:
            a = v[:, lo - 5120 : lo - 5120 + WK]
        part = jnp.dot(a, wbuf[i % 3], preferred_element_type=F32)
        pre[...] = part if i == 0 else pre[...] + part

    def pass_on(n):
        pair = kg.at[pl.ds(y * 8 + lax.rem(row // 2 + 4 - n, 4) * 2, 2)]
        for m in (2, 1, 3):
            c = remote(
                pair, pair, ys.at[n * 4 + m], yr.at[n * 4 + m],
                (lax.rem(y + m, 4) * 8 + row, x),
            )
            c.start()
            yc.append(c)

    own_k.wait()
    for n in range(4):
        for c in kc[n]:
            c.wait_recv()
        pass_on(n)
        if n < KW:
            multiply(n)
    for i in range(KW, chunks):
        multiply(i)
    for c in qc + fc + yc:
        c.wait()
    for cs in kc:
        for c in cs:
            c.wait_send()
    own_q.wait()
    for c in own_f:
        c.wait()


def spread(q, k, v, w):
    dma = pltpu.SemaphoreType.DMA
    vmem = pl.BlockSpec(memory_space=VM)
    hbm = pl.BlockSpec(memory_space=pltpu.HBM)
    return pl.pallas_call(
        spread_kernel,
        name="spread",
        out_shape=(
            jax.ShapeDtypeStruct((8, 128, 512), BF16),
            jax.ShapeDtypeStruct((32, 128, 128), BF16),
            jax.ShapeDtypeStruct((16, 48, 1024), BF16),
            jax.ShapeDtypeStruct((128, 1024), F32),
        ),
        in_specs=[vmem, vmem, vmem, hbm],
        out_specs=(vmem,) * 4,
        scratch_shapes=[
            VM((16, 8, 48, 128), BF16),
            VM((3, WK, 1024), BF16),
            dma((3,)),
            dma((8,)), dma((8,)), dma((8,)), dma((8,)),
            dma((8 * FP,)), dma((8 * FP,)), dma((16,)), dma((16,)),
            dma((2 + FP,)),
        ],
        compiler_params=pltpu.CompilerParams(
            collective_id=0, has_side_effects=True, vmem_limit_bytes=40 * 2**20
        ),
    )(q, k, v, w)


def mass_kernel(meta, length, qg, kg, out, live, kpos, s_ref, acc):
    seq, _, y, _, _ = place()
    limit = length[0]
    first = y * 8
    here = lax.broadcasted_iota(jnp.int32, (1, 128), 1) + meta[seq] * 128
    live[...] = (here < limit).astype(F32)
    factor = math.log2(math.e) / math.sqrt(128)

    def order(r, _):
        for t in range(8):
            kpos[pl.ds(pl.multiple_of(meta[r * 8 + t] * 128, 128), 128)] = kg[r * 8 + t]
        return 0

    lax.fori_loop(0, 4, order, 0)
    acc[...] = jnp.zeros_like(acc)
    lane = lax.rem(lax.broadcasted_iota(jnp.int32, (1, 512), 1), 128)
    sub = lax.broadcasted_iota(jnp.int32, (CK, 512), 0)

    def fold(a, op):
        return op(a.reshape(a.shape[0] // 8, 8, 512), axis=0)

    def block(i, _):
        pos = meta[first + i]

        @pl.when(pos * 128 < limit)
        def _():
            last = pos * 128 // CK
            big = lax.rem(pos, CK // 128) // (CK // 256)
            q4 = jnp.concatenate([qg[i, :, h * 128 : (h + 1) * 128] for h in range(4)], axis=0)

            def span(size, c):
                return pl.ds(pl.multiple_of(c * CK, CK), size)

            def first_pass(size, masked, c, top):
                rows = span(size, c)
                s = lax.dot_general(
                    kpos[rows], q4, (((1,), (1,)), ((), ())), preferred_element_type=F32
                )
                if masked:
                    s = jnp.where(sub[0:size] <= lane + (pos * 128 - c * CK), s, -1e30)
                s_ref[rows] = s
                return jnp.maximum(top, fold(s, jnp.max))

            def run(step, state):
                state = lax.fori_loop(0, last + big, functools.partial(step, CK), state)
                return lax.fori_loop(
                    last + big, last + 1, functools.partial(step, CK // 2), state
                )

            top = jnp.full((8, 512), -1e30, F32)
            top = lax.fori_loop(0, last, functools.partial(first_pass, CK, False), top)
            top = lax.fori_loop(
                last, last + big, functools.partial(first_pass, CK, True), top
            )
            top = lax.fori_loop(
                last + big, last + 1, functools.partial(first_pass, CK // 2, True), top
            )
            top = jnp.max(top, axis=0, keepdims=True)

            def second_pass(size, c, total):
                rows = span(size, c)
                e = jnp.exp2((s_ref[rows] - top) * factor)
                s_ref[rows] = e
                return total + fold(e, jnp.sum)

            total = jnp.sum(run(second_pass, jnp.zeros((8, 512), F32)), axis=0, keepdims=True)
            share = jnp.where(lane + pos * 128 < limit, 1.0 / total, 0.0)

            def third_pass(size, c, _):
                rows = span(size, c)
                e = s_ref[rows] * share
                acc[rows] += (e[:, 0:128] + e[:, 128:256]) + (e[:, 256:384] + e[:, 384:512])
                return 0

            run(third_pass, 0)

        return 0

    lax.fori_loop(0, 8, block, 0)

    def give(r, _):
        for t in range(16):
            rows = acc[pl.ds(pl.multiple_of(meta[r * 16 + t] * 128, 128), 128)]
            out[pl.ds(r * 16 + t, 1)] = jnp.sum(rows.T, axis=0, keepdims=True)
        return 0

    lax.fori_loop(0, 2, give, 0)


def column_mass(order, length, qg, kg):
    smem = pl.BlockSpec(memory_space=pltpu.SMEM)
    vmem = pl.BlockSpec(memory_space=VM)
    return pl.pallas_call(
        mass_kernel,
        name="column_mass",
        out_shape=(jax.ShapeDtypeStruct((32, 128), F32), jax.ShapeDtypeStruct((1, 128), F32)),
        in_specs=[smem, smem, vmem, vmem],
        out_specs=(vmem, vmem),
        scratch_shapes=[VM((4096, 128), BF16), VM((4096, 512), F32), VM((4096, 128), F32)],
        compiler_params=pltpu.CompilerParams(vmem_limit_bytes=40 * 2**20),
    )(order, length, qg, kg)


def reduce_kernel(
    norm, mass, pre, b_in, wo, bo, live, ft, out, small,
    m1, m2s, m2, dl, gs, res, rs, ps, ts, pk, p1, p2, p3,
    s1, r1, s2, r2, s3, r3, s4, r4, s5, r5, s6, r6, s7, r7, s8, r8, s9, r9,
):
    seq, x, y, row, core = place()
    z = row // 2
    j = group_rank(x, core)
    greet(seq, x, y, row, core)()

    def y_dev(n):
        return (lax.rem(y + n, 4) * 8 + row, x)

    def z_dev(n):
        return (y * 8 + lax.rem(z + n, 4) * 2 + core, x)

    cs = []
    for n in range(1, 4):
        c = remote(mass.at[lax.rem(y + n, 4)], m1.at[y], s1.at[n], r1.at[n], y_dev(n))
        c.start()
        cs.append(c)
    m1[y] = mass[y]
    lin = pre[...] + b_in[...]
    sig = jax.nn.sigmoid(lin)
    act = (lin * sig).astype(BF16)
    slope = sig * (1.0 + lin * (1.0 - sig))
    wide_o = jnp.concatenate([wo[...], jnp.zeros((120, 1024), BF16)], axis=0)
    for c in cs:
        c.wait()
    total = (m1[0] + m1[1]) + (m1[2] + m1[3])
    for i in range(8):
        m2s[i] = jnp.broadcast_to(total[i : i + 1], (8, 128))
    cs = []
    for n in range(1, 8):
        to = lax.rem(row + n, 8)
        c = remote(m2s.at[to], m2.at[row], s2.at[n], r2.at[n], (y * 8 + to, x))
        c.start()
        cs.append(c)
    m2[row] = m2s[row]
    p8 = lax.dot_general(wide_o, act, (((1,), (1,)), ((), ())), preferred_element_type=F32)
    pred = jnp.concatenate([p8[g : g + 1] + bo[g] for g in range(8)], axis=0)
    for c in cs:
        c.wait()
    mass_t = jnp.concatenate([m2[g, 0:1] for g in range(8)], axis=0)
    label = jnp.log1p(mass_t)
    resid = ((pred - label) * live[...] * norm).astype(BF16).astype(F32)
    wide = jnp.concatenate([resid, jnp.zeros((120, 128), F32)], axis=0)
    back = jnp.dot(wide.T.astype(BF16), wide_o, preferred_element_type=F32)
    delta = (back * slope).astype(BF16)
    other = (seq + 1 - 2 * core, x)
    base = core * 4
    for h in range(8):
        dl[h, j] = delta[:, h * 128 : (h + 1) * 128]
    parts = len(PARTS)

    def give(p, slot, n, dev):
        some = dl.at[pl.ds(PARTS[p][0], len(PARTS[p])), slot]
        return remote(some, some, s3.at[p * 8 + n], r3.at[p * 8 + n], dev)

    direct = [[give(p, j, n, (seq, lax.rem(x + n, 4))) for n in (2, 1, 3)] for p in range(parts)]
    passed = [
        [give(p, base + lax.rem(x + 4 - n, 4), 4 + n, other) for n in (0, 2, 1, 3)]
        for p in range(parts)
    ]

    def set_out(p):
        for c in direct[p]:
            c.start()
        passed[p][0].start()

    set_out(0)
    term = jnp.dot(wide.astype(BF16), act, preferred_element_type=F32)[0:8]
    bias = jnp.sum(delta.astype(F32), axis=0, keepdims=True)
    for i in range(4):
        pk[i] = term[:, i * 256 : (i + 1) * 256]
    pk[4, :, 0:128] = resid
    for i in range(8):
        pk[4, i : i + 1, 128:256] = bias[:, i * 128 : (i + 1) * 128]
    for i in range(5, 8):
        pk[i] = jnp.zeros((8, 256), F32)
    xs = []
    for n in range(1, 8):
        c = remote(
            pk.at[lax.rem(j + n, 8)], p1.at[j], s4.at[n], r4.at[n], group_peer(seq, x, core, n)
        )
        c.start()
        xs.append(c)
    p1[j] = pk[j]
    for p in range(1, parts):
        set_out(p)

    first, second = [], []

    def fold(h):
        for c in first[h]:
            c.wait()
        if h % 2 == 0:
            t = res[h, y]
            for n in range(1, 4):
                t = t + rs[h, lax.rem(y + n, 4)].astype(F32)
        else:
            t = res[h, :, z]
            for n in range(1, 4):
                t = t + rs[h, lax.rem(z + n, 4)].astype(F32)
        ps[h] = t
        cs = []
        for n in (2, 1, 3):
            if h % 2 == 0:
                c = remote(
                    ps.at[h, lax.rem(z + n, 4)], ts.at[h, z],
                    s9.at[h * 4 + n], r9.at[h * 4 + n], z_dev(n),
                )
            else:
                c = remote(
                    ps.at[h, lax.rem(y + n, 4)], ts.at[h, y],
                    s9.at[h * 4 + n], r9.at[h * 4 + n], y_dev(n),
                )
            c.start()
            cs.append(c)
        second.append(cs)

    f_all = ft[...].reshape(768, 1024)
    for p in range(parts):
        for c, d in zip(direct[p], passed[p][1:]):
            c.wait_recv()
            d.start()
        if p >= 2:
            for h in PARTS[p - 2]:
                fold(h)
        for c in passed[p]:
            c.wait_recv()
        d_all = jnp.concatenate([dl[h].reshape(1024, 128) for h in PARTS[p]], axis=1)
        g = jnp.dot(f_all, d_all, preferred_element_type=F32)
        for i, h in enumerate(PARTS[p]):
            half = g[:, i * 128 : (i + 1) * 128].reshape(4, 4, 48, 128)
            gs[h] = half.astype(BF16)
            res[h] = half
            cs = []
            for n in (2, 1, 3):
                if h % 2 == 0:
                    c = remote(
                        gs.at[h, lax.rem(y + n, 4)], rs.at[h, y],
                        s8.at[h * 4 + n], r8.at[h * 4 + n], y_dev(n),
                    )
                else:
                    c = remote(
                        gs.at[h, :, lax.rem(z + n, 4)], rs.at[h, z],
                        s8.at[h * 4 + n], r8.at[h * 4 + n], z_dev(n),
                    )
                c.start()
                cs.append(c)
            first.append(cs)
        if p == 0:
            for c in xs:
                c.wait()
            t = p1[0]
            for i in range(1, 8):
                t = t + p1[i]
            p2[y] = t
            sy = []
            for n in range(1, 4):
                c = remote(p2.at[y], p2.at[y], s5.at[n], r5.at[n], y_dev(n))
                c.start()
                sy.append(c)
        if p == 2:
            for c in sy:
                c.wait()
            p3[z] = (p2[0] + p2[1]) + (p2[2] + p2[3])
            zs = []
            for n in range(1, 4):
                c = remote(p3.at[z], p3.at[z], s6.at[n], r6.at[n], z_dev(n))
                c.start()
                zs.append(c)
        if p == 3:
            for c in zs:
                c.wait()
            small[j] = (p3[0] + p3[1]) + (p3[2] + p3[3])
            fin = []
            for n in range(1, 8):
                c = remote(
                    small.at[j], small.at[j], s7.at[n], r7.at[n], group_peer(seq, x, core, n)
                )
                c.start()
                fin.append(c)
    for h in PARTS[parts - 2] + PARTS[parts - 1]:
        fold(h)
    for p in range(parts):
        for c in direct[p] + passed[p]:
            c.wait_send()
    for h in range(8):
        for c in second[h]:
            c.wait()
        if h % 2 == 0:
            t = ps[h, z]
            for n in range(1, 4):
                t = t + ts[h, lax.rem(z + n, 4)]
        else:
            t = ps[h, y]
            for n in range(1, 4):
                t = t + ts[h, lax.rem(y + n, 4)]
        out[:, h * 128 : (h + 1) * 128] = t
    for c in fin:
        c.wait()


def reduce_all(norm, mass, pre, b_in, wo, bo, live, ft):
    dma = pltpu.SemaphoreType.DMA
    vmem = pl.BlockSpec(memory_space=VM)
    smem = pl.BlockSpec(memory_space=pltpu.SMEM)
    return pl.pallas_call(
        functools.partial(reduce_kernel, norm),
        name="reduce_all",
        out_shape=(
            jax.ShapeDtypeStruct((48, 1024), F32),
            jax.ShapeDtypeStruct((8, 8, 256), F32),
        ),
        in_specs=[vmem, vmem, vmem, vmem, smem, vmem, vmem],
        out_specs=(vmem,) * 2,
        scratch_shapes=[
            VM((4, 8, 128), F32), VM((8, 8, 128), F32), VM((8, 8, 128), F32),
            VM((8, 8, 128, 128), BF16),
            VM((8, 4, 4, 48, 128), BF16),
            VM((8, 4, 4, 48, 128), F32),
            VM((8, 4, 4, 48, 128), BF16),
            VM((8, 4, 48, 128), F32),
            VM((8, 4, 48, 128), F32),
            VM((8, 8, 256), F32), VM((8, 8, 256), F32), VM((4, 8, 256), F32), VM((4, 8, 256), F32),
        ]
        + [dma((4,)), dma((4,)), dma((8,)), dma((8,)), dma((40,)), dma((40,)), dma((8,)), dma((8,))]
        + [dma((4,)), dma((4,)), dma((4,)), dma((4,)), dma((8,)), dma((8,))]
        + [dma((32,)), dma((32,)), dma((32,)), dma((32,))],
        compiler_params=pltpu.CompilerParams(
            collective_id=1, has_side_effects=True, vmem_limit_bytes=40 * 2**20
        ),
    )(mass, pre, b_in, wo, bo, live, ft)


def finish_kernel(g, small, grad, bias, term, last):
    grad[...] = g[...]
    bias[...] = small[4, :, 128:256]
    t = jnp.concatenate([small[i] for i in range(4)], axis=1)
    term[...] = t
    r = jnp.concatenate([small[4, :, 0:128], jnp.zeros((120, 128), F32)], axis=0).T
    last[...] = jnp.sum(r, axis=0, keepdims=True)[:, 0:8]


def finish(g, small):
    vmem = pl.BlockSpec(memory_space=VM)
    return pl.pallas_call(
        finish_kernel,
        name="finish",
        out_shape=(
            jax.ShapeDtypeStruct((48, 1024), F32),
            jax.ShapeDtypeStruct((8, 128), F32),
            jax.ShapeDtypeStruct((8, 1024), F32),
            jax.ShapeDtypeStruct((1, 8), F32),
        ),
        in_specs=[vmem] * 2,
        out_specs=(vmem,) * 4,
        compiler_params=pltpu.CompilerParams(vmem_limit_bytes=8 * 2**20),
    )(g, small)


def on_device(queries, keys, values, lengths, block_pos, w_in, b_in, output_weight, output_bias):
    norm = 1.0 / math.sqrt(4 * 4096)
    qg, kg, ft, pre = spread(queries[0], keys[0], values[0], w_in)
    mass, live = column_mass(block_pos[0], lengths, qg, kg)
    g, small = reduce_all(
        norm, mass.reshape(4, 8, 128), pre, b_in[None, :], output_weight.T, output_bias, live, ft
    )
    grad, bias, term, last = finish(g, small)
    return (grad, bias.reshape(1024), term.T, last.reshape(8))


def solution(mesh):
    return jax.shard_map(
        on_device,
        mesh=mesh,
        in_specs=(
            P("batch", "seq", None),
            P("batch", "seq", None),
            P("batch", "seq", None),
            P("batch"),
            P("batch", None),
            P(),
            P(),
            P(),
            P(),
        ),
        out_specs=(P(("seq", "batch"), None), P(), P(), P()),
        check_vma=False,
    )
```
